16 devices in a mesh: terms: 16 (over z, y, x, core).
Axes of the slice: x: 2, y: 2, z: 2, core: 2. Of those that a mesh axis runs over, the one named last changes fastest.
Arguments:
- wavefunction: float32 [384, 16, 384], replicated
- left_env: bfloat16 [64, 384, 384], P('terms')
- pair_ops: bfloat16 [64, 16, 16], P('terms')
- right_env: bfloat16 [64, 384, 384], P('terms')
- full_term: int32 [64], P('terms')
Outputs:
- output 1: float32 [7, 384, 16, 384], P(None, 'terms')
- output 2: float32 [6], replicated
- output 3: float32 [6], replicated
All inputs are finite; a program needn't handle non-finite values.
Results may differ from the reference program's by a relative error of at most 0.0127149.
Values are sent between devices in bfloat16 or wider.
A program may use at most 1 GiB of HBM per device.

```python
import jax
import jax.numpy as jnp
from jax import lax

BOND_DIM = 384
PHYS_DIM = 4
TERMS_DEV = 4
NUM_DEV = 16
NUM_TERMS = 64
LANCZOS_STEPS = 6

PAIR_DIM = PHYS_DIM * PHYS_DIM
VEC_SIZE = BOND_DIM * PAIR_DIM * BOND_DIM


def normal_sym(rng_key, num_mats, mat_size):
    raw_draw = jax.random.normal(rng_key, (num_mats, mat_size, mat_size), jnp.float32)
    return (raw_draw + jnp.swapaxes(raw_draw, 1, 2)) * (2.0 * mat_size) ** -0.5


def draw_flags(rng_key):
    count_key, pick_key, order_key = jax.random.split(rng_key, 3)
    block_counts = jax.random.randint(count_key, (NUM_DEV,), 0, TERMS_DEV + 1)
    picked = jax.random.permutation(pick_key, NUM_DEV)
    block_counts = block_counts.at[picked[0]].set(TERMS_DEV).at[picked[1]].set(0)
    rank_table = jax.vmap(lambda sub_key: jax.random.permutation(sub_key, TERMS_DEV))(jax.random.split(order_key, NUM_DEV))
    return (rank_table < block_counts[:, None]).astype(jnp.int32).reshape(NUM_TERMS)


def setup_inputs(seed: int = 0) -> dict:
    wave_key, left_key, pair_key, right_key, flag_key = jax.random.split(jax.random.key(seed), 5)
    diag_shift = (2.0 / NUM_TERMS ** 0.5) ** 0.5
    wavefunction = jax.random.normal(wave_key, (BOND_DIM, PAIR_DIM, BOND_DIM), jnp.float32)
    left_env = (normal_sym(left_key, NUM_TERMS, BOND_DIM) + diag_shift * jnp.eye(BOND_DIM, dtype=jnp.float32)).astype(jnp.bfloat16)
    pair_ops = ((normal_sym(pair_key, NUM_TERMS, PAIR_DIM) + diag_shift * jnp.eye(PAIR_DIM, dtype=jnp.float32)) * NUM_TERMS ** -0.5).astype(jnp.bfloat16)
    right_env = normal_sym(right_key, NUM_TERMS, BOND_DIM).astype(jnp.bfloat16)
    full_term = draw_flags(flag_key)
    return {'wavefunction': wavefunction, 'left_env': left_env, 'pair_ops': pair_ops, 'right_env': right_env, 'full_term': full_term}


def apply_term(vec_bf, term_data):
    left_env, pair_op, right_env, flag_val = term_data
    flat_vec = vec_bf.reshape(BOND_DIM * PAIR_DIM, BOND_DIM)
    right_done = jnp.dot(flat_vec, right_env.T, preferred_element_type=jnp.float32).astype(jnp.bfloat16)
    right_done = jnp.where(flag_val == 1, right_done.reshape(BOND_DIM, PAIR_DIM, BOND_DIM), vec_bf)
    pair_in = right_done.transpose(1, 0, 2).reshape(PAIR_DIM, BOND_DIM * BOND_DIM)
    pair_done = jnp.dot(pair_op, pair_in, preferred_element_type=jnp.float32).astype(jnp.bfloat16)
    left_in = pair_done.reshape(PAIR_DIM, BOND_DIM, BOND_DIM).transpose(1, 0, 2).reshape(BOND_DIM, PAIR_DIM * BOND_DIM)
    return jnp.dot(left_env, left_in, preferred_element_type=jnp.float32).reshape(BOND_DIM, PAIR_DIM, BOND_DIM)


def apply_hamiltonian(vector, left_env, pair_ops, right_env, full_term):
    vec_bf = vector.astype(jnp.bfloat16)

    def add_term(running_sum, term_data):
        return running_sum + apply_term(vec_bf, term_data), None

    start_sum = jnp.zeros((BOND_DIM, PAIR_DIM, BOND_DIM), jnp.float32)
    total_sum, unused = lax.scan(add_term, start_sum, (left_env, pair_ops, right_env, full_term))
    return total_sum


def reference(wavefunction, left_env, pair_ops, right_env, full_term):
    first_vec = wavefunction / jnp.sqrt(jnp.sum(wavefunction * wavefunction) / VEC_SIZE)

    def lanczos_step(state_in, unused):
        current, previous, beta_prev = state_in
        sigma_vec = apply_hamiltonian(current, left_env, pair_ops, right_env, full_term)
        alpha_now = jnp.sum(sigma_vec * current) / VEC_SIZE
        residual = sigma_vec - alpha_now * current - beta_prev * previous
        beta_now = jnp.sqrt(jnp.sum(residual * residual) / VEC_SIZE)
        following = residual / beta_now
        return (following, current, beta_now), (following, alpha_now, beta_now)

    start_state = (first_vec, jnp.zeros_like(first_vec), jnp.zeros((), jnp.float32))
    final_state, outputs = lax.scan(lanczos_step, start_state, None, length=LANCZOS_STEPS)
    vectors, alpha_diag, beta_offdiag = outputs
    krylov = jnp.concatenate([first_vec[None], vectors], axis=0)
    return krylov, alpha_diag, beta_offdiag
```

```python
import functools

import jax
import jax.numpy as jnp
from jax import lax
from jax.experimental import pallas as pl
from jax.experimental.pallas import tpu as pltpu
from jax.sharding import PartitionSpec as P

STEPS = 6
AXIS = 'terms'
BOND = 384
PAIR = 16
VEC_SIZE = BOND * PAIR * BOND
CHIPS = 8
COLS = BOND // CHIPS
HALF = PAIR // 2
KLOC = 4
CHUNK = 128
NCHUNK = BOND // CHUNK
QROWS = HALF * COLS
ROWS = BOND // 16
MESH = pl.DeviceIdType.MESH
F32 = jnp.float32
BF16 = jnp.bfloat16
PEERS = (1, 2, 4, 3, 5, 6, 7)


def flip(idx, mask, bits):
    out = 0
    for b in range(bits):
        bit = lax.rem(lax.div(idx, 1 << b), 2)
        if (mask >> b) & 1:
            bit = 1 - bit
        out = out + bit * (1 << b)
    return out


def rotl(pos, chunk):
    scaled = pos * (1 + chunk + lax.div(chunk, 2)) if not isinstance(chunk, int) else pos * (1 << chunk)
    return scaled - 7 * lax.div(scaled, 8)


def kernel(u0_ref, v0_ref, l_ref, r_ref, w_ref,
           kry_ref, alpha_ref, beta_ref,
           u, lbuf, rbuf, wbuf, mbuf, ybuf, zbuf, sig, sig_in, wv, vcur, vprev, tbuf, red, beta_prev,
           loc_sem, rs_sem, rr_sem, ws_sem, wr_sem, ls_sem, lr_sem, gs_sem, gr_sem, fs_sem, fr_sem,
           xs_sem, xr_sem, ds_sem, dr_sem, ks_sem, kr_sem, kl_sem):
    me = lax.axis_index(AXIS)
    chip = lax.div(me, 2)
    core = lax.rem(me, 2)
    partner = flip(me, 1, 4)

    def peer(d):
        return flip(chip, d, 3) * 2 + core

    def remote(src, dst, ssem, rsem, dev):
        return pltpu.make_async_remote_copy(src_ref=src, dst_ref=dst, send_sem=ssem, recv_sem=rsem,
                                            device_id=(dev,), device_id_type=MESH)

    local = [pltpu.make_async_copy(l_ref.at[i], lbuf.at[i, pl.ds(0, 512)], loc_sem.at[i]) for i in range(NCHUNK)]
    local.append(pltpu.make_async_copy(u0_ref, u, loc_sem.at[3]))
    local.append(pltpu.make_async_copy(r_ref.at[:, pl.ds(pl.multiple_of(COLS * chip, 16), COLS)], rbuf.at[0], loc_sem.at[4]))
    for c in local:
        c.start()
    barrier = pltpu.get_barrier_semaphore()
    for d in range(1, 16):
        pl.semaphore_signal(barrier, inc=1, device_id=(flip(me, d, 4),), device_id_type=MESH)
    pl.semaphore_wait(barrier, 15)

    w_copies = {d: remote(w_ref, wbuf.at[d], ws_sem.at[d], wr_sem.at[d], peer(d)) for d in PEERS}
    r_copies = {d: remote(r_ref.at[:, pl.ds(pl.multiple_of(COLS * flip(chip, d, 3), 16), COLS)], rbuf.at[d],
                          rs_sem.at[d], rr_sem.at[d], peer(d)) for d in PEERS}

    def l_copy(i, n):
        mask = 1 << ((i + min(n, 2)) % 3)
        src, dst, size = ((0, 512, 512), (0, 1024, 1024), (0, 2048, 1024), (1024, 3072, 1024))[n]
        return remote(lbuf.at[i, pl.ds(src, size)], lbuf.at[i, pl.ds(dst, size)], ls_sem.at[i, n], lr_sem.at[i, n], peer(mask))

    for d in PEERS:
        w_copies[d].start()
    for d in (1, 2, 4):
        r_copies[d].start()
    for i in range(NCHUNK):
        local[i].wait()
        l_copy(i, 0).start()
    for d in (3, 5, 6, 7):
        r_copies[d].start()

    wbuf[0] = w_ref[...]
    for d in PEERS:
        w_copies[d].wait_recv()
    row_id = lax.broadcasted_iota(jnp.int32, (256, 16), 0)
    col_id = lax.broadcasted_iota(jnp.int32, (256, 16), 1)
    spread = jnp.where(lax.div(row_id, 16) == col_id, 1.0, 0.0).astype(BF16)
    row_id = lax.broadcasted_iota(jnp.int32, (128, 256), 0)
    col_id = lax.broadcasted_iota(jnp.int32, (128, 256), 1)
    spread_t = jnp.where(row_id == lax.div(col_id, 16), 1.0, 0.0).astype(BF16)
    row_id = lax.broadcasted_iota(jnp.int32, (256, 256), 0)
    col_id = lax.broadcasted_iota(jnp.int32, (256, 256), 1)
    same = lax.rem(row_id, 16) == lax.rem(col_id, 16)

    def build(slot, carry):
        for k in range(KLOC):
            tall = jnp.dot(spread, wbuf[slot, pl.ds(16 * k, 16), :], preferred_element_type=F32).astype(BF16)
            full = jnp.dot(tall, spread_t, preferred_element_type=F32)
            mbuf[slot * KLOC + k] = jnp.where(same, full, 0.0).astype(BF16)
        return carry

    lax.fori_loop(0, CHIPS, build, 0)

    def group(i, g):
        slot_a = rotl(2 * g, i)
        slot_b = rotl(2 * g + 1, i)
        right = jnp.concatenate([rbuf[slot_a].reshape(KLOC * COLS, BOND), rbuf[slot_b].reshape(KLOC * COLS, BOND)], axis=0)
        for n in range(8):
            lanes = pl.ds(256 * n, 256)
            ybuf[:, lanes] = jnp.dot(right, u[i, :, lanes], preferred_element_type=F32).astype(BF16)
        for kk in range(8):
            mat = mbuf[(slot_a if kk < KLOC else slot_b) * KLOC + kk % KLOC]
            cols = [jnp.concatenate([ybuf[COLS * kk + 16 * t:COLS * kk + 16 * t + 16, 128 * r:128 * r + 128]
                                     for r in range(PAIR)], axis=0) for t in range(3)]
            pair = jnp.dot(mat, jnp.concatenate(cols, axis=1), preferred_element_type=F32).astype(BF16)
            for q in range(PAIR):
                for t in range(3):
                    zbuf[COLS * q + 16 * t:COLS * q + 16 * t + 16, 128 * kk:128 * kk + 128] = \
                        pair[16 * q:16 * q + 16, 128 * t:128 * t + 128]
        left = lbuf[i, pl.ds(pl.multiple_of(g * 1024, 1024), 1024), :]
        sig[...] += jnp.dot(zbuf[...], left, preferred_element_type=F32)

    def all_sum(phase, part):
        red[phase, me] = part
        copies = []
        for d in range(1, 16):
            c = remote(red.at[phase, me], red.at[phase, me], ds_sem.at[phase, d], dr_sem.at[phase, d], flip(me, d, 4))
            c.start()
            copies.append(c)
        for c in copies:
            c.wait_recv()
        total = red[phase, 0]
        for s in range(1, 16):
            total = total + red[phase, s]
        for c in copies:
            c.wait_send()
        return jnp.sum(total, keepdims=True) / VEC_SIZE

    def fold(x):
        out = x[0:8, 0:128]
        for r in range(COLS // 8):
            for c in range(NCHUNK):
                if r or c:
                    out = out + x[8 * r:8 * r + 8, 128 * c:128 * c + 128]
        return out

    def vector_part(j):
        theirs = sig.at[pl.ds(pl.multiple_of(QROWS * (1 - core), QROWS), QROWS)]
        swap = remote(theirs, sig_in, xs_sem, xr_sem, partner)
        swap.start()
        swap.wait_recv()
        part = jnp.zeros((8, 128), F32)
        for q in range(HALF):
            rows = pl.ds(COLS * q, COLS)
            w = sig[pl.ds(pl.multiple_of(QROWS * core + COLS * q, COLS), COLS), :] + sig_in[rows, :]
            wv[rows, :] = w
            part = part + fold(w * vcur[rows, :])
        alpha = all_sum(0, part)
        beta_old = beta_prev[0:1, 0:1]
        part = jnp.zeros((8, 128), F32)
        for q in range(HALF):
            rows = pl.ds(COLS * q, COLS)
            w = wv[rows, :] - alpha * vcur[rows, :] - beta_old * vprev[rows, :]
            wv[rows, :] = w
            part = part + fold(w * w)
        beta = jnp.sqrt(all_sum(1, part))
        for q in range(HALF):
            rows = pl.ds(COLS * q, COLS)
            vprev[rows, :] = vcur[rows, :]
            vcur[rows, :] = wv[rows, :] / beta
        beta_prev[...] = jnp.broadcast_to(beta, (8, 128))
        alpha_ref[j] = jnp.broadcast_to(alpha, (8, 128))
        beta_ref[j] = jnp.broadcast_to(beta, (8, 128))
        swap.wait_send()

    def kry_copies(j):
        return [remote(tbuf.at[pl.ds(pl.multiple_of(ROWS * flip(me, d, 4), 8), ROWS)], kry_ref.at[j, me],
                       ks_sem.at[d], kr_sem.at[d], flip(me, d, 4)) for d in range(1, 16)]

    def kry_own(j):
        return pltpu.make_async_copy(tbuf.at[pl.ds(pl.multiple_of(ROWS * me, 8), ROWS)], kry_ref.at[j, me], kl_sem)

    def kry_start(j):
        tbuf[...] = vcur[...].T
        kry_own(j).start()
        for c in kry_copies(j):
            c.start()

    def kry_wait(j):
        kry_own(j).wait()
        for c in kry_copies(j):
            c.wait()

    vcur[...] = v0_ref[...]
    vprev[...] = jnp.zeros_like(vprev)
    beta_prev[...] = jnp.zeros_like(beta_prev)
    sig[...] = jnp.zeros_like(sig)
    local[3].wait()
    local[4].wait()
    for d in (1, 2, 4):
        r_copies[d].wait_recv()
    for i in range(NCHUNK):
        l_copy(i, 0).wait_recv()
        l_copy(i, 1).start()

    def first_body(idx, carry):
        g = lax.div(idx, 3)
        i = lax.rem(idx, 3)

        @pl.when(idx == 3)
        def _():
            for d in (3, 5, 6, 7):
                r_copies[d].wait_recv()
            for c in range(NCHUNK):
                l_copy(c, 1).wait_recv()
                l_copy(c, 2).start()
            for c in range(NCHUNK):
                l_copy(c, 3).start()

        @pl.when(idx == 6)
        def _():
            for c in range(NCHUNK):
                l_copy(c, 2).wait_recv()

        @pl.when(idx == 9)
        def _():
            for c in range(NCHUNK):
                l_copy(c, 3).wait_recv()

        group(i, g)
        return carry

    lax.fori_loop(0, 12, first_body, 0)
    for d in PEERS:
        w_copies[d].wait_send()
        r_copies[d].wait_send()
    for i in range(NCHUNK):
        for n in range(4):
            l_copy(i, n).wait_send()
    vector_part(0)

    def region(i, c):
        return u.at[i, pl.ds(pl.multiple_of(COLS * c, 16), COLS), pl.ds(pl.multiple_of(HALF * CHUNK * core, 1024), HALF * CHUNK)]

    def gather(i, d):
        return remote(region(i, chip), region(i, chip), gs_sem.at[i, d], gr_sem.at[i, d], peer(d))

    def forward(i, d):
        src = region(i, flip(chip, d, 3))
        return remote(src, src, fs_sem.at[i, d], fr_sem.at[i, d], partner)

    def relay(i):
        for d in PEERS:
            gather(i, d).wait_recv()
            forward(i, d).start()

    def step_body(j, carry):
        for q in range(HALF):
            val = vcur[COLS * q:COLS * q + COLS, :].astype(BF16)
            for i in range(NCHUNK):
                u[i, pl.ds(pl.multiple_of(COLS * chip, 16), COLS),
                  pl.ds(pl.multiple_of(HALF * CHUNK * core + CHUNK * q, 128), CHUNK)] = val[:, CHUNK * i:CHUNK * i + CHUNK]
        for i in range(NCHUNK):
            for d in PEERS:
                gather(i, d).start()
            forward(i, 0).start()
        kry_start(j - 1)
        sig[...] = jnp.zeros_like(sig)
        relay(0)

        def body(idx, carry):
            i = lax.div(idx, 4)
            g = lax.rem(idx, 4)

            for c in range(NCHUNK):
                @pl.when(idx == 4 * c)
                def _():
                    for d in range(8):
                        forward(c, d).wait_recv()
            for c in range(1, NCHUNK):
                @pl.when(idx == 4 * c - 1)
                def _():
                    relay(c)

            group(i, g)
            return carry

        lax.fori_loop(0, 12, body, 0)
        for i in range(NCHUNK):
            forward(i, 0).wait_send()
            for d in PEERS:
                gather(i, d).wait_send()
                forward(i, d).wait_send()
        kry_wait(j - 1)
        vector_part(j)
        return carry

    lax.fori_loop(1, STEPS, step_body, 0)
    kry_start(STEPS - 1)
    kry_wait(STEPS - 1)


def matvec_steps(u0, v0, l_in, r_in, w_in):
    dma = pltpu.SemaphoreType.DMA
    vmem = pl.BlockSpec(memory_space=pltpu.VMEM)
    hbm = pl.BlockSpec(memory_space=pl.ANY)
    return pl.pallas_call(
        kernel,
        out_shape=(jax.ShapeDtypeStruct((STEPS, 16, ROWS, BOND), F32),
                   jax.ShapeDtypeStruct((STEPS, 8, 128), F32),
                   jax.ShapeDtypeStruct((STEPS, 8, 128), F32)),
        in_specs=[hbm, vmem, hbm, hbm, vmem],
        out_specs=(hbm, vmem, vmem),
        scratch_shapes=[
            pltpu.VMEM((NCHUNK, BOND, PAIR * CHUNK), BF16),
            pltpu.VMEM((NCHUNK, CHIPS * KLOC * CHUNK, BOND), BF16),
            pltpu.VMEM((CHIPS, KLOC, COLS, BOND), BF16),
            pltpu.VMEM((CHIPS, KLOC * 16, 128), BF16),
            pltpu.VMEM((CHIPS * KLOC, 256, 256), BF16),
            pltpu.VMEM((2 * KLOC * COLS, PAIR * CHUNK), BF16),
            pltpu.VMEM((PAIR * COLS, 2 * KLOC * CHUNK), BF16),
            pltpu.VMEM((PAIR * COLS, BOND), F32),
            pltpu.VMEM((QROWS, BOND), F32),
            pltpu.VMEM((QROWS, BOND), F32),
            pltpu.VMEM((QROWS, BOND), F32),
            pltpu.VMEM((QROWS, BOND), F32),
            pltpu.VMEM((BOND, QROWS), F32),
            pltpu.VMEM((2, 16, 8, 128), F32),
            pltpu.VMEM((8, 128), F32),
            dma((5,)), dma((8,)), dma((8,)), dma((8,)), dma((8,)),
            dma((NCHUNK, 4)), dma((NCHUNK, 4)),
            dma((NCHUNK, 8)), dma((NCHUNK, 8)), dma((NCHUNK, 8)), dma((NCHUNK, 8)),
            dma, dma, dma((2, 16)), dma((2, 16)), dma((16,)), dma((16,)), dma,
        ],
        compiler_params=pltpu.CompilerParams(collective_id=0, has_side_effects=True, vmem_limit_bytes=60 * 1024 * 1024),
        name='lanczos',
    )(u0, v0, l_in, r_in, w_in)


def solution(mesh):
    def device_body(psi, left_loc, pair_loc, right_loc, flag_loc):
        me = lax.axis_index(AXIS)
        chip, core = me // 2, me % 2
        norm = jnp.sqrt(jnp.sum(psi * psi) / VEC_SIZE)
        first_rows = lax.dynamic_slice_in_dim(psi, me * ROWS, ROWS, axis=0) / norm
        u0 = (psi / norm).astype(BF16).reshape(NCHUNK, CHUNK, PAIR, BOND).transpose(0, 3, 2, 1).reshape(NCHUNK, BOND, PAIR * CHUNK)
        v0 = lax.dynamic_slice(psi, (0, core * HALF, chip * COLS), (BOND, HALF, COLS)) / norm
        v0 = v0.transpose(1, 2, 0).reshape(QROWS, BOND)
        l_in = left_loc.reshape(KLOC, NCHUNK, CHUNK, BOND).transpose(1, 0, 2, 3).reshape(NCHUNK, KLOC * CHUNK, BOND)
        eye = jnp.eye(BOND, dtype=BF16)
        r_in = jnp.where((flag_loc == 1)[:, None, None], right_loc, eye)
        w_in = jnp.pad(pair_loc.reshape(KLOC * PAIR, PAIR), ((0, 0), (0, 128 - PAIR)))
        blocks, alpha, beta = matvec_steps(u0, v0, l_in, r_in, w_in)
        rest = blocks.reshape(STEPS, CHIPS, 2, ROWS, HALF, COLS).transpose(0, 3, 2, 4, 1, 5).reshape(STEPS, ROWS, PAIR, BOND)
        return jnp.concatenate([first_rows[None], rest], axis=0), alpha[:, 0, 0], beta[:, 0, 0]

    return jax.shard_map(device_body, mesh=mesh, in_specs=(P(), P(AXIS), P(AXIS), P(AXIS), P(AXIS)),
                         out_specs=(P(None, AXIS), P(), P()), check_vma=False)
```

```python
import jax
import jax.numpy as jnp
from jax import lax
from jax.experimental import pallas as pl
from jax.experimental.pallas import tpu as pltpu
from jax.sharding import PartitionSpec as P

STEPS = 6
AXIS = 'terms'
BOND = 384
PAIR = 16
VEC_SIZE = BOND * PAIR * BOND
CHIPS = 8
COLS = BOND // CHIPS
HALF = PAIR // 2
KLOC = 4
CHUNK = 128
NCHUNK = BOND // CHUNK
QROWS = HALF * COLS
ROWS = BOND // 16
MESH = pl.DeviceIdType.MESH
F32 = jnp.float32
BF16 = jnp.bfloat16
PEERS = (1, 2, 4, 3, 5, 6, 7)


def flip(idx, mask, bits):
    out = 0
    for b in range(bits):
        bit = lax.rem(lax.div(idx, 1 << b), 2)
        if (mask >> b) & 1:
            bit = 1 - bit
        out = out + bit * (1 << b)
    return out


def rotl(pos, chunk):
    scaled = pos * (1 + chunk + lax.div(chunk, 2)) if not isinstance(chunk, int) else pos * (1 << chunk)
    return scaled - 7 * lax.div(scaled, 8)


def kernel(psi_ref, l_ref, r_ref, w_ref,
           kry_ref, alpha_ref, beta_ref, first_ref,
           psi, u, lbuf, rbuf, wbuf, mbuf, ybuf, zbuf, sig, sig_in, wv, vcur, vprev, tbuf, red, beta_prev,
           psi_sem, ll_sem, loc_sem, rs_sem, rr_sem, ws_sem, wr_sem, ls_sem, lr_sem, gs_sem, gr_sem, fs_sem, fr_sem,
           xs_sem, xr_sem, ds_sem, dr_sem, ks_sem, kr_sem, kl_sem):
    me = lax.axis_index(AXIS)
    chip = lax.div(me, 2)
    core = lax.rem(me, 2)
    partner = flip(me, 1, 4)

    def peer(d):
        return flip(chip, d, 3) * 2 + core

    def remote(src, dst, ssem, rsem, dev):
        return pltpu.make_async_remote_copy(src_ref=src, dst_ref=dst, send_sem=ssem, recv_sem=rsem,
                                            device_id=(dev,), device_id_type=MESH)

    l_own = [[pltpu.make_async_copy(l_ref.at[k, pl.ds(CHUNK * i, CHUNK)], lbuf.at[i, pl.ds(CHUNK * k, CHUNK)], ll_sem.at[i, k])
              for k in range(KLOC)] for i in range(NCHUNK)]
    r_own = pltpu.make_async_copy(r_ref.at[:, pl.ds(pl.multiple_of(COLS * chip, 16), COLS)], rbuf.at[0], loc_sem)
    part_rows = BOND * PAIR // 4
    psi_own = [[pltpu.make_async_copy(psi_ref.at[pl.ds(part_rows * i, part_rows), pl.ds(128 * c, 128)],
                                      psi.at[c, pl.ds(part_rows * i, part_rows)], psi_sem.at[i, c]) for c in range(3)]
               for i in range(4)]
    for i in range(NCHUNK):
        for k in range(KLOC):
            l_own[i][k].start()
    r_own.start()
    for i in range(4):
        for c in range(3):
            psi_own[i][c].start()
    barrier = pltpu.get_barrier_semaphore()
    for d in range(1, 16):
        pl.semaphore_signal(barrier, inc=1, device_id=(flip(me, d, 4),), device_id_type=MESH)
    pl.semaphore_wait(barrier, 15)

    w_copies = {d: remote(w_ref, wbuf.at[d], ws_sem.at[d], wr_sem.at[d], peer(d)) for d in PEERS}
    r_copies = {d: remote(r_ref.at[:, pl.ds(pl.multiple_of(COLS * flip(chip, d, 3), 16), COLS)], rbuf.at[d],
                          rs_sem.at[d], rr_sem.at[d], peer(d)) for d in PEERS}

    def l_copy(i, n):
        mask = 1 << ((i + min(n, 2)) % 3)
        src, dst, size = ((0, 512, 512), (0, 1024, 1024), (0, 2048, 1024), (1024, 3072, 1024))[n]
        return remote(lbuf.at[i, pl.ds(src, size)], lbuf.at[i, pl.ds(dst, size)], ls_sem.at[i, n], lr_sem.at[i, n], peer(mask))

    for d in PEERS:
        w_copies[d].start()
    for d in (1, 2, 4):
        r_copies[d].start()
    for i in range(NCHUNK):
        for k in range(KLOC):
            l_own[i][k].wait()
        l_copy(i, 0).start()
    for d in (3, 5, 6, 7):
        r_copies[d].start()

    wbuf[0] = w_ref[...]
    for d in PEERS:
        w_copies[d].wait_recv()
    row_id = lax.broadcasted_iota(jnp.int32, (256, 16), 0)
    col_id = lax.broadcasted_iota(jnp.int32, (256, 16), 1)
    spread = jnp.where(lax.div(row_id, 16) == col_id, 1.0, 0.0).astype(BF16)
    row_id = lax.broadcasted_iota(jnp.int32, (128, 256), 0)
    col_id = lax.broadcasted_iota(jnp.int32, (128, 256), 1)
    spread_t = jnp.where(row_id == lax.div(col_id, 16), 1.0, 0.0).astype(BF16)
    row_id = lax.broadcasted_iota(jnp.int32, (256, 256), 0)
    col_id = lax.broadcasted_iota(jnp.int32, (256, 256), 1)
    same = lax.rem(row_id, 16) == lax.rem(col_id, 16)

    def build(slot, carry):
        for k in range(KLOC):
            tall = jnp.dot(spread, wbuf[slot, pl.ds(16 * k, 16), :], preferred_element_type=F32).astype(BF16)
            full = jnp.dot(tall, spread_t, preferred_element_type=F32)
            mbuf[slot * KLOC + k] = jnp.where(same, full, 0.0).astype(BF16)
        return carry

    lax.fori_loop(0, CHIPS, build, 0)

    def group(i, g):
        slot_a = rotl(2 * g, i)
        slot_b = rotl(2 * g + 1, i)
        right = jnp.concatenate([rbuf[slot_a].reshape(KLOC * COLS, BOND), rbuf[slot_b].reshape(KLOC * COLS, BOND)], axis=0)
        for n in range(8):
            lanes = pl.ds(256 * n, 256)
            ybuf[:, lanes] = jnp.dot(right, u[i, :, lanes], preferred_element_type=F32).astype(BF16)
        for kk in range(8):
            mat = mbuf[(slot_a if kk < KLOC else slot_b) * KLOC + kk % KLOC]
            cols = [jnp.concatenate([ybuf[COLS * kk + 16 * t:COLS * kk + 16 * t + 16, 128 * r:128 * r + 128]
                                     for r in range(PAIR)], axis=0) for t in range(3)]
            pair = jnp.dot(mat, jnp.concatenate(cols, axis=1), preferred_element_type=F32).astype(BF16)
            for q in range(PAIR):
                for t in range(3):
                    zbuf[COLS * q + 16 * t:COLS * q + 16 * t + 16, 128 * kk:128 * kk + 128] = \
                        pair[16 * q:16 * q + 16, 128 * t:128 * t + 128]
        left = lbuf[i, pl.ds(pl.multiple_of(g * 1024, 1024), 1024), :]
        sig[...] += jnp.dot(zbuf[...], left, preferred_element_type=F32)

    def all_sum(phase, part):
        red[phase, me] = part
        copies = []
        for d in range(1, 16):
            c = remote(red.at[phase, me], red.at[phase, me], ds_sem.at[phase, d], dr_sem.at[phase, d], flip(me, d, 4))
            c.start()
            copies.append(c)
        for c in copies:
            c.wait_recv()
        total = red[phase, 0]
        for s in range(1, 16):
            total = total + red[phase, s]
        for c in copies:
            c.wait_send()
        return jnp.sum(total, keepdims=True) / VEC_SIZE

    def fold(x):
        out = x[0:8, 0:128]
        for r in range(COLS // 8):
            for c in range(NCHUNK):
                if r or c:
                    out = out + x[8 * r:8 * r + 8, 128 * c:128 * c + 128]
        return out

    def vector_part(j):
        theirs = sig.at[pl.ds(pl.multiple_of(QROWS * (1 - core), QROWS), QROWS)]
        swap = remote(theirs, sig_in, xs_sem, xr_sem, partner)
        swap.start()
        swap.wait_recv()
        part = jnp.zeros((8, 128), F32)
        for q in range(HALF):
            rows = pl.ds(COLS * q, COLS)
            w = sig[pl.ds(pl.multiple_of(QROWS * core + COLS * q, COLS), COLS), :] + sig_in[rows, :]
            wv[rows, :] = w
            part = part + fold(w * vcur[rows, :])
        alpha = all_sum(0, part)
        beta_old = beta_prev[0:1, 0:1]
        part = jnp.zeros((8, 128), F32)
        for q in range(HALF):
            rows = pl.ds(COLS * q, COLS)
            w = wv[rows, :] - alpha * vcur[rows, :] - beta_old * vprev[rows, :]
            wv[rows, :] = w
            part = part + fold(w * w)
        beta = jnp.sqrt(all_sum(1, part))
        for q in range(HALF):
            rows = pl.ds(COLS * q, COLS)
            vprev[rows, :] = vcur[rows, :]
            vcur[rows, :] = wv[rows, :] / beta
        beta_prev[...] = jnp.broadcast_to(beta, (8, 128))
        alpha_ref[j] = jnp.broadcast_to(alpha, (8, 128))
        beta_ref[j] = jnp.broadcast_to(beta, (8, 128))
        swap.wait_send()

    def kry_copies(j):
        return [remote(tbuf.at[pl.ds(pl.multiple_of(ROWS * flip(me, d, 4), 8), ROWS)], kry_ref.at[j, me],
                       ks_sem.at[d], kr_sem.at[d], flip(me, d, 4)) for d in range(1, 16)]

    def kry_own(j):
        return pltpu.make_async_copy(tbuf.at[pl.ds(pl.multiple_of(ROWS * me, 8), ROWS)], kry_ref.at[j, me], kl_sem)

    def kry_start(j):
        tbuf[...] = vcur[...].T
        kry_own(j).start()
        for c in kry_copies(j):
            c.start()

    def kry_wait(j):
        kry_own(j).wait()
        for c in kry_copies(j):
            c.wait()

    square = jnp.zeros((8, 128), F32)
    for i in range(4):
        for c in range(3):
            psi_own[i][c].wait()

        def add_squares(n, acc, base=i * part_rows):
            for c in range(3):
                x = psi[c, pl.ds(pl.multiple_of(base + COLS * n, COLS), COLS), :]
                x = x * x
                for r in range(COLS // 8):
                    acc = acc + x[8 * r:8 * r + 8, :]
            return acc

        square = lax.fori_loop(0, part_rows // COLS, add_squares, square)
    norm = jnp.sqrt(jnp.sum(square, keepdims=True) / VEC_SIZE)

    def spread_pair(q, carry):
        for i in range(NCHUNK):
            for c in range(NCHUNK):
                x = psi[c, pl.ds(CHUNK * PAIR * i + q, CHUNK, stride=PAIR), :]
                x = (x / norm).T
                u[i, pl.ds(128 * c, 128), pl.ds(pl.multiple_of(CHUNK * q, CHUNK), CHUNK)] = x.astype(BF16)
                tbuf[pl.ds(128 * c, 128), pl.ds(CHUNK * i, CHUNK)] = x

        @pl.when(lax.div(q, HALF) == core)
        def _():
            vcur[pl.ds(pl.multiple_of(COLS * lax.rem(q, HALF), COLS), COLS), :] = tbuf[pl.ds(pl.multiple_of(COLS * chip, COLS), COLS), :]

        return carry

    lax.fori_loop(0, PAIR, spread_pair, 0)

    def first_rows(n, carry):
        for c in range(3):
            first_ref[pl.ds(pl.multiple_of(COLS * n, COLS), COLS), pl.ds(128 * c, 128)] = \
                psi[c, pl.ds(pl.multiple_of(ROWS * PAIR * me + COLS * n, COLS), COLS), :] / norm
        return carry

    lax.fori_loop(0, ROWS * PAIR // COLS, first_rows, 0)

    vprev[...] = jnp.zeros_like(vprev)
    beta_prev[...] = jnp.zeros_like(beta_prev)
    sig[...] = jnp.zeros_like(sig)
    r_own.wait()
    for d in (1, 2, 4):
        r_copies[d].wait_recv()
    for i in range(NCHUNK):
        l_copy(i, 0).wait_recv()
        l_copy(i, 1).start()

    def first_body(idx, carry):
        g = lax.div(idx, 3)
        i = lax.rem(idx, 3)

        @pl.when(idx == 3)
        def _():
            for d in (3, 5, 6, 7):
                r_copies[d].wait_recv()
            for c in range(NCHUNK):
                l_copy(c, 1).wait_recv()
                l_copy(c, 2).start()
            for c in range(NCHUNK):
                l_copy(c, 3).start()

        @pl.when(idx == 6)
        def _():
            for c in range(NCHUNK):
                l_copy(c, 2).wait_recv()

        @pl.when(idx == 9)
        def _():
            for c in range(NCHUNK):
                l_copy(c, 3).wait_recv()

        group(i, g)
        return carry

    lax.fori_loop(0, 12, first_body, 0)
    for d in PEERS:
        w_copies[d].wait_send()
        r_copies[d].wait_send()
    for i in range(NCHUNK):
        for n in range(4):
            l_copy(i, n).wait_send()
    vector_part(0)

    def region(i, c):
        return u.at[i, pl.ds(pl.multiple_of(COLS * c, 16), COLS), pl.ds(pl.multiple_of(HALF * CHUNK * core, 1024), HALF * CHUNK)]

    def gather(i, d):
        return remote(region(i, chip), region(i, chip), gs_sem.at[i, d], gr_sem.at[i, d], peer(d))

    def forward(i, d):
        src = region(i, flip(chip, d, 3))
        return remote(src, src, fs_sem.at[i, d], fr_sem.at[i, d], partner)

    def relay(i):
        for d in PEERS:
            gather(i, d).wait_recv()
            forward(i, d).start()

    def step_body(j, carry):
        for q in range(HALF):
            val = vcur[COLS * q:COLS * q + COLS, :].astype(BF16)
            for i in range(NCHUNK):
                u[i, pl.ds(pl.multiple_of(COLS * chip, 16), COLS),
                  pl.ds(pl.multiple_of(HALF * CHUNK * core + CHUNK * q, 128), CHUNK)] = val[:, CHUNK * i:CHUNK * i + CHUNK]
        for i in range(NCHUNK):
            for d in PEERS:
                gather(i, d).start()
            forward(i, 0).start()
        kry_start(j - 1)
        sig[...] = jnp.zeros_like(sig)
        relay(0)

        def body(idx, carry):
            i = lax.div(idx, 4)
            g = lax.rem(idx, 4)

            for c in range(NCHUNK):
                @pl.when(idx == 4 * c)
                def _():
                    for d in range(8):
                        forward(c, d).wait_recv()
            for c in range(1, NCHUNK):
                @pl.when(idx == 4 * c - 1)
                def _():
                    relay(c)

            group(i, g)
            return carry

        lax.fori_loop(0, 12, body, 0)
        for i in range(NCHUNK):
            forward(i, 0).wait_send()
            for d in PEERS:
                gather(i, d).wait_send()
                forward(i, d).wait_send()
        kry_wait(j - 1)
        vector_part(j)
        return carry

    lax.fori_loop(1, STEPS, step_body, 0)
    kry_start(STEPS - 1)
    kry_wait(STEPS - 1)


def run_steps(psi, left_loc, r_in, w_in):
    dma = pltpu.SemaphoreType.DMA
    vmem = pl.BlockSpec(memory_space=pltpu.VMEM)
    hbm = pl.BlockSpec(memory_space=pl.ANY)
    return pl.pallas_call(
        kernel,
        out_shape=(jax.ShapeDtypeStruct((STEPS, 16, ROWS, BOND), F32),
                   jax.ShapeDtypeStruct((STEPS, 8, 128), F32),
                   jax.ShapeDtypeStruct((STEPS, 8, 128), F32),
                   jax.ShapeDtypeStruct((ROWS * PAIR, BOND), F32)),
        in_specs=[hbm, hbm, hbm, vmem],
        out_specs=(hbm, vmem, vmem, vmem),
        scratch_shapes=[
            pltpu.VMEM((3, BOND * PAIR, 128), F32),
            pltpu.VMEM((NCHUNK, BOND, PAIR * CHUNK), BF16),
            pltpu.VMEM((NCHUNK, CHIPS * KLOC * CHUNK, BOND), BF16),
            pltpu.VMEM((CHIPS, KLOC, COLS, BOND), BF16),
            pltpu.VMEM((CHIPS, KLOC * 16, 128), BF16),
            pltpu.VMEM((CHIPS * KLOC, 256, 256), BF16),
            pltpu.VMEM((2 * KLOC * COLS, PAIR * CHUNK), BF16),
            pltpu.VMEM((PAIR * COLS, 2 * KLOC * CHUNK), BF16),
            pltpu.VMEM((PAIR * COLS, BOND), F32),
            pltpu.VMEM((QROWS, BOND), F32),
            pltpu.VMEM((QROWS, BOND), F32),
            pltpu.VMEM((QROWS, BOND), F32),
            pltpu.VMEM((QROWS, BOND), F32),
            pltpu.VMEM((BOND, QROWS), F32),
            pltpu.VMEM((2, 16, 8, 128), F32),
            pltpu.VMEM((8, 128), F32),
            dma((4, 3)), dma((NCHUNK, KLOC)), dma, dma((8,)), dma((8,)), dma((8,)), dma((8,)),
            dma((NCHUNK, 4)), dma((NCHUNK, 4)),
            dma((NCHUNK, 8)), dma((NCHUNK, 8)), dma((NCHUNK, 8)), dma((NCHUNK, 8)),
            dma, dma, dma((2, 16)), dma((2, 16)), dma((16,)), dma((16,)), dma,
        ],
        compiler_params=pltpu.CompilerParams(collective_id=0, has_side_effects=True, vmem_limit_bytes=60 * 1024 * 1024),
        name='lanczos',
    )(psi, left_loc, r_in, w_in)


def place_kernel(first_ref, block_ref, out_ref):
    j = pl.program_id(0)

    @pl.when(j == 0)
    def _():
        out_ref[0] = first_ref[...]

    @pl.when(j > 0)
    def _():
        for h in range(2):
            for q in range(HALF):
                pieces = [block_ref[0, 2 * c + h, :, COLS * q:COLS * q + COLS] for c in range(CHIPS)]
                out_ref[0, :, HALF * h + q, :] = jnp.concatenate(pieces, axis=1)


def place_rows(first, blocks):
    return pl.pallas_call(
        place_kernel,
        grid=(STEPS + 1,),
        out_shape=jax.ShapeDtypeStruct((STEPS + 1, ROWS, PAIR, BOND), F32),
        in_specs=[pl.BlockSpec((ROWS, PAIR, BOND), lambda j: (0, 0, 0)),
                  pl.BlockSpec((1, 16, ROWS, BOND), lambda j: (jnp.maximum(j - 1, 0), 0, 0, 0))],
        out_specs=pl.BlockSpec((1, ROWS, PAIR, BOND), lambda j: (j, 0, 0, 0)),
        name='place_rows',
    )(first, blocks)


def solution(mesh):
    def device_body(psi, left_loc, pair_loc, right_loc, flag_loc):
        r_in = jnp.where((flag_loc == 1)[:, None, None], right_loc, jnp.eye(BOND, dtype=BF16))
        w_in = jnp.pad(pair_loc.reshape(KLOC * PAIR, PAIR), ((0, 0), (0, 128 - PAIR)))
        blocks, alpha, beta, first = run_steps(psi.reshape(BOND * PAIR, BOND), left_loc, r_in, w_in)
        krylov = place_rows(first.reshape(ROWS, PAIR, BOND), blocks)
        return krylov, alpha[:, 0, 0], beta[:, 0, 0]

    return jax.shard_map(device_body, mesh=mesh, in_specs=(P(), P(AXIS), P(AXIS), P(AXIS), P(AXIS)),
                         out_specs=(P(None, AXIS), P(), P()), check_vma=False)
```

```python
import jax
import jax.numpy as jnp
from jax import lax
from jax.experimental import pallas as pl
from jax.experimental.pallas import tpu as pltpu
from jax.sharding import PartitionSpec as P

STEPS = 6
AXIS = 'terms'
BOND = 384
PAIR = 16
VEC_SIZE = BOND * PAIR * BOND
CHIPS = 8
COLS = BOND // CHIPS
HALF = PAIR // 2
KLOC = 4
CHUNK = 128
NCHUNK = BOND // CHUNK
QROWS = HALF * COLS
ROWS = BOND // 16
MESH = pl.DeviceIdType.MESH
F32 = jnp.float32
BF16 = jnp.bfloat16
PEERS = (1, 2, 4, 3, 5, 6, 7)
FORWARD_AT = 3


def flip(idx, mask, bits):
    out = 0
    for b in range(bits):
        bit = lax.rem(lax.div(idx, 1 << b), 2)
        if (mask >> b) & 1:
            bit = 1 - bit
        out = out + bit * (1 << b)
    return out


def rotl(pos, chunk):
    scaled = pos * (1 + chunk + lax.div(chunk, 2)) if not isinstance(chunk, int) else pos * (1 << chunk)
    return scaled - 7 * lax.div(scaled, 8)


def kernel(psi_ref, l_ref, r_ref, w_ref,
           kry_ref, alpha_ref, beta_ref, first_ref,
           psi, u, lbuf, rbuf, wbuf, mbuf, ya, yb, z, sig, sig_in, wv, vcur, vprev, red, norm_v, delta_now, beta_now,
           psi_sem, ll_sem, loc_sem, rs_sem, rr_sem, ws_sem, wr_sem, ls_sem, lr_sem, gs_sem, gr_sem, fs_sem, fr_sem,
           xs_sem, xr_sem, ds_sem, dr_sem, ks_sem, kr_sem, kl_sem):
    me = lax.axis_index(AXIS)
    chip = lax.div(me, 2)
    core = lax.rem(me, 2)
    partner = flip(me, 1, 4)

    def peer(d):
        return flip(chip, d, 3) * 2 + core

    def remote(src, dst, ssem, rsem, dev):
        return pltpu.make_async_remote_copy(src_ref=src, dst_ref=dst, send_sem=ssem, recv_sem=rsem,
                                            device_id=(dev,), device_id_type=MESH)

    l_own = [[pltpu.make_async_copy(l_ref.at[k, :, pl.ds(CHUNK * i, CHUNK)], lbuf.at[i, :, pl.ds(CHUNK * k, CHUNK)], ll_sem.at[i, k])
              for k in range(KLOC)] for i in range(NCHUNK)]
    r_own = pltpu.make_async_copy(r_ref.at[:, pl.ds(pl.multiple_of(COLS * chip, 16), COLS)], rbuf.at[0], loc_sem)
    part_rows = BOND * PAIR // 4
    psi_own = [[pltpu.make_async_copy(psi_ref.at[pl.ds(part_rows * i, part_rows), pl.ds(128 * c, 128)],
                                      psi.at[c, pl.ds(part_rows * i, part_rows)], psi_sem.at[i, c]) for c in range(3)]
               for i in range(4)]
    for i in range(NCHUNK):
        for k in range(KLOC):
            l_own[i][k].start()
    r_own.start()
    for i in range(4):
        for c in range(3):
            psi_own[i][c].start()
    barrier = pltpu.get_barrier_semaphore()
    for d in range(1, 16):
        pl.semaphore_signal(barrier, inc=1, device_id=(flip(me, d, 4),), device_id_type=MESH)
    pl.semaphore_wait(barrier, 15)

    w_copies = {d: remote(w_ref, wbuf.at[d], ws_sem.at[d], wr_sem.at[d], peer(d)) for d in PEERS}
    r_copies = {d: remote(r_ref.at[:, pl.ds(pl.multiple_of(COLS * flip(chip, d, 3), 16), COLS)], rbuf.at[d],
                          rs_sem.at[d], rr_sem.at[d], peer(d)) for d in PEERS}

    def l_copies(i, n):
        mask = 1 << ((i + min(n, 2)) % 3)
        src, dst, size = ((0, 512, 512), (0, 1024, 1024), (0, 2048, 1024), (1024, 3072, 1024))[n]
        spans = ((CHUNK * i, 2 * CHUNK),) if i < 2 else ((2 * CHUNK, CHUNK), (0, CHUNK))
        return [remote(lbuf.at[i, pl.ds(row, num), pl.ds(src, size)], lbuf.at[i, pl.ds(row, num), pl.ds(dst, size)],
                       ls_sem.at[i, n, m], lr_sem.at[i, n, m], peer(mask)) for m, (row, num) in enumerate(spans)]

    def l_start(i, n):
        for c in l_copies(i, n):
            c.start()

    def l_wait(i, n):
        for c in l_copies(i, n):
            c.wait_recv()

    for d in PEERS:
        w_copies[d].start()
    for d in (1, 2, 4):
        r_copies[d].start()
    for i in range(NCHUNK):
        for k in range(KLOC):
            l_own[i][k].wait()
        l_start(i, 0)
    for d in (3, 5, 6, 7):
        r_copies[d].start()

    wbuf[0] = w_ref[...]
    for d in PEERS:
        w_copies[d].wait_recv()
    row_id = lax.broadcasted_iota(jnp.int32, (256, 16), 0)
    col_id = lax.broadcasted_iota(jnp.int32, (256, 16), 1)
    spread = jnp.where(lax.div(row_id, 16) == col_id, 1.0, 0.0).astype(BF16)
    row_id = lax.broadcasted_iota(jnp.int32, (128, 256), 0)
    col_id = lax.broadcasted_iota(jnp.int32, (128, 256), 1)
    spread_t = jnp.where(row_id == lax.div(col_id, 16), 1.0, 0.0).astype(BF16)
    row_id = lax.broadcasted_iota(jnp.int32, (256, 256), 0)
    col_id = lax.broadcasted_iota(jnp.int32, (256, 256), 1)
    same = lax.rem(row_id, 16) == lax.rem(col_id, 16)

    def build(slot, carry):
        for k in range(KLOC):
            tall = jnp.dot(spread, wbuf[slot, pl.ds(16 * k, 16), :], preferred_element_type=F32).astype(BF16)
            full = jnp.dot(tall, spread_t, preferred_element_type=F32)
            mbuf[slot * KLOC + k] = jnp.where(same, full, 0.0).astype(BF16)
        return carry

    lax.fori_loop(0, CHIPS, build, 0)

    def right_part(i, g, y):
        slot_a = rotl(2 * g, i)
        slot_b = rotl(2 * g + 1, i)
        right = jnp.concatenate([rbuf[slot_a].reshape(KLOC * COLS, BOND), rbuf[slot_b].reshape(KLOC * COLS, BOND)], axis=0)
        for n in range(8):
            lanes = pl.ds(256 * n, 256)
            y[:, lanes] = jnp.dot(right, u[i, :, lanes], preferred_element_type=F32).astype(BF16)

    def pair_part(i, g, y, slot):
        slot_a = rotl(2 * g, i)
        slot_b = rotl(2 * g + 1, i)
        for kk in range(8):
            mat = mbuf[(slot_a if kk < KLOC else slot_b) * KLOC + kk % KLOC]
            cols = [jnp.concatenate([y[COLS * kk + 16 * t:COLS * kk + 16 * t + 16, 128 * r:128 * r + 128]
                                     for r in range(PAIR)], axis=0) for t in range(3)]
            pair = jnp.dot(mat, jnp.concatenate(cols, axis=1), preferred_element_type=F32).astype(BF16)
            for q in range(PAIR):
                for t in range(3):
                    z[slot, COLS * q + 16 * t:COLS * q + 16 * t + 16, 128 * kk:128 * kk + 128] = \
                        pair[16 * q:16 * q + 16, 128 * t:128 * t + 128]

    def left_part(i, g, slot):
        left = lbuf[i, :, pl.ds(pl.multiple_of(g * 1024, 1024), 1024)]
        sig[...] += lax.dot_general(left, z[slot], (((1,), (1,)), ((), ())), preferred_element_type=F32)

    def fold(x):
        out = x[0:8, 0:128]
        for r in range(COLS // 8):
            for c in range(NCHUNK):
                if r or c:
                    out = out + x[8 * r:8 * r + 8, 128 * c:128 * c + 128]
        return out

    def total(x):
        return jnp.sum(x, keepdims=True)

    def vector_part(j):
        lanes = pl.ds(pl.multiple_of(QROWS * core, 128), QROWS)
        swap = remote(sig.at[:, pl.ds(pl.multiple_of(QROWS * (1 - core), 128), QROWS)], sig_in, xs_sem, xr_sem, partner)
        swap.start()
        beta_old = beta_now[0:1, 0:1]
        swap.wait_recv()
        s_wv = jnp.zeros((8, 128), F32)
        s_cv = jnp.zeros((8, 128), F32)
        for n in range(BOND // COLS):
            rows = pl.ds(COLS * n, COLS)
            w = sig[rows, lanes] + sig_in[rows, :]
            v = vcur[rows, :]
            s_wv = s_wv + fold(w * v)
            w = w - beta_old * vprev[rows, :]
            s_cv = s_cv + fold(w * v)
            wv[rows, :] = w
        s_vv = total(norm_v[...])
        guess = jnp.where(s_vv > 0.0, total(s_cv) / jnp.where(s_vv > 0.0, s_vv, 1.0), 0.0)
        s_ww = jnp.zeros((8, 128), F32)
        s_w2v = jnp.zeros((8, 128), F32)
        for n in range(BOND // COLS):
            rows = pl.ds(COLS * n, COLS)
            v = vcur[rows, :]
            w = wv[rows, :] - guess * v
            wv[rows, :] = w
            s_ww = s_ww + fold(w * w)
            s_w2v = s_w2v + fold(w * v)
        row_of = lax.broadcasted_iota(jnp.int32, (8, 128), 0)
        message = jnp.where(row_of == 0, total(s_wv),
                            jnp.where(row_of == 1, guess,
                                      jnp.where(row_of == 2, s_vv, jnp.where(row_of == 3, total(s_ww), total(s_w2v)))))
        phase = lax.rem(j, 2)
        mine = pl.ds(pl.multiple_of(8 * me, 8), 8)
        red[phase, mine, :] = message
        copies = [remote(red.at[phase, mine], red.at[phase, mine], ds_sem.at[phase, d], dr_sem.at[phase, d], flip(me, d, 4))
                  for d in range(1, 16)]
        for c in copies:
            c.start()
        for c in copies:
            c.wait_recv()
        table = red.at[phase]
        a_wv, a_guess, a_vv, a_ww, a_w2v = [table[pl.ds(r, 16, stride=8), :] for r in range(5)]
        alpha = jnp.sum(a_wv, axis=0, keepdims=True) / VEC_SIZE
        shift = alpha - a_guess
        beta = jnp.sqrt(jnp.sum(a_ww - 2.0 * shift * a_w2v + shift * shift * a_vv, axis=0, keepdims=True) / VEC_SIZE)
        beta_now[...] = jnp.broadcast_to(beta, (8, 128))
        delta_now[...] = jnp.broadcast_to(alpha[0:1, 0:1] - guess, (8, 128))
        alpha_ref[j] = jnp.broadcast_to(alpha, (8, 128))
        beta_ref[j] = jnp.broadcast_to(beta, (8, 128))
        norm_v[...] = jnp.zeros_like(norm_v)
        for c in copies:
            c.wait_send()
        swap.wait_send()

    def advance(i):
        beta = beta_now[0:1, 0:1]
        delta = delta_now[0:1, 0:1]
        rows = pl.ds(CHUNK * i, CHUNK)
        old = vcur[rows, :]
        new = (wv[rows, :] - delta * old) / beta
        vprev[rows, :] = old
        vcur[rows, :] = new
        square = new * new
        acc = norm_v[...]
        for r in range(CHUNK // 8):
            for c in range(NCHUNK):
                acc = acc + square[8 * r:8 * r + 8, 128 * c:128 * c + 128]
        norm_v[...] = acc
        return new

    def kry_copies(j):
        return [remote(vcur.at[pl.ds(pl.multiple_of(ROWS * flip(me, d, 4), 8), ROWS)], kry_ref.at[j, me],
                       ks_sem.at[d], kr_sem.at[d], flip(me, d, 4)) for d in range(1, 16)]

    def kry_own(j):
        return pltpu.make_async_copy(vcur.at[pl.ds(pl.multiple_of(ROWS * me, 8), ROWS)], kry_ref.at[j, me], kl_sem)

    def kry_start(j):
        kry_own(j).start()
        for c in kry_copies(j):
            c.start()

    def kry_wait(j):
        kry_own(j).wait()
        for c in kry_copies(j):
            c.wait()

    square = jnp.zeros((8, 128), F32)
    for i in range(4):
        for c in range(3):
            psi_own[i][c].wait()

        def add_squares(n, acc, base=i * part_rows):
            for c in range(3):
                x = psi[c, pl.ds(pl.multiple_of(base + COLS * n, COLS), COLS), :]
                x = x * x
                for r in range(COLS // 8):
                    acc = acc + x[8 * r:8 * r + 8, :]
            return acc

        square = lax.fori_loop(0, part_rows // COLS, add_squares, square)
    norm = jnp.sqrt(jnp.sum(square, keepdims=True) / VEC_SIZE)

    def spread_pair(q, carry):
        for i in range(NCHUNK):
            for c in range(NCHUNK):
                x = psi[c, pl.ds(CHUNK * PAIR * i + q, CHUNK, stride=PAIR), :]
                x = (x / norm).T
                u[i, pl.ds(128 * c, 128), pl.ds(pl.multiple_of(CHUNK * q, CHUNK), CHUNK)] = x.astype(BF16)
                wv[pl.ds(128 * c, 128), pl.ds(CHUNK * i, CHUNK)] = x

        @pl.when(lax.div(q, HALF) == core)
        def _():
            sig[pl.ds(pl.multiple_of(COLS * lax.rem(q, HALF), COLS), COLS), 0:BOND] = wv[pl.ds(pl.multiple_of(COLS * chip, COLS), COLS), :]

        return carry

    lax.fori_loop(0, PAIR, spread_pair, 0)
    start = jnp.zeros((8, 128), F32)
    for i in range(NCHUNK):
        x = sig[:, pl.ds(CHUNK * i, CHUNK)].T
        vcur[pl.ds(CHUNK * i, CHUNK), :] = x
        x = x * x
        for r in range(CHUNK // 8):
            for c in range(NCHUNK):
                start = start + x[8 * r:8 * r + 8, 128 * c:128 * c + 128]
    norm_v[...] = start

    def first_rows(n, carry):
        for c in range(3):
            first_ref[pl.ds(pl.multiple_of(COLS * n, COLS), COLS), pl.ds(128 * c, 128)] = \
                psi[c, pl.ds(pl.multiple_of(ROWS * PAIR * me + COLS * n, COLS), COLS), :] / norm
        return carry

    lax.fori_loop(0, ROWS * PAIR // COLS, first_rows, 0)

    vprev[...] = jnp.zeros_like(vprev)
    beta_now[...] = jnp.zeros_like(beta_now)
    sig[...] = jnp.zeros_like(sig)
    r_own.wait()
    for i in range(NCHUNK):
        l_wait(i, 0)
        l_start(i, 1)
    for d in PEERS:
        r_copies[d].wait_recv()

    def front_body(n, carry):
        @pl.when(n == FORWARD_AT)
        def _():
            for i in range(NCHUNK):
                l_wait(i, 1)
                l_start(i, 2)
            for i in range(NCHUNK):
                l_start(i, 3)

        i = lax.div(n, 2)
        g = 2 * lax.rem(n, 2)
        right_part(i, g, ya)
        right_part(i, g + 1, yb)
        pair_part(i, g, ya, 4 * i + g)
        pair_part(i, g + 1, yb, 4 * i + g + 1)
        return carry

    lax.fori_loop(0, 6, front_body, 0)

    def mirror(i, g):
        other = lax.rem(i + 2, 3)
        for k in range(2):
            slot = rotl(2 * g + k, i)
            pos = rotl(slot, lax.rem(3 - other, 3))
            for n in range(KLOC):
                block = lbuf[other, pl.ds(pl.multiple_of(CHUNK * i, CHUNK), CHUNK),
                             pl.ds(pl.multiple_of(CHUNK * (KLOC * pos + n), CHUNK), CHUNK)]
                lbuf[i, pl.ds(pl.multiple_of(CHUNK * other, CHUNK), CHUNK),
                     pl.ds(pl.multiple_of(CHUNK * (KLOC * (2 * g + k) + n), CHUNK), CHUNK)] = block.T

    def back(g):
        def body(i, carry):
            mirror(i, g)
            left_part(i, g, 4 * i + g)
            return carry

        lax.fori_loop(0, NCHUNK, body, 0)

    back(0)
    for i in range(NCHUNK):
        l_wait(i, 2)
    back(2)
    for i in range(NCHUNK):
        l_wait(i, 3)
    back(1)
    back(3)
    for d in PEERS:
        w_copies[d].wait_send()
        r_copies[d].wait_send()
    for i in range(NCHUNK):
        for n in range(4):
            for c in l_copies(i, n):
                c.wait_send()
    vector_part(0)

    def region(i, c):
        return u.at[i, pl.ds(pl.multiple_of(COLS * c, 16), COLS), pl.ds(pl.multiple_of(HALF * CHUNK * core, 1024), HALF * CHUNK)]

    def gather(i, d):
        return remote(region(i, chip), region(i, chip), gs_sem.at[i, d], gr_sem.at[i, d], peer(d))

    def forward(i, d):
        src = region(i, flip(chip, d, 3))
        return remote(src, src, fs_sem.at[i, d], fr_sem.at[i, d], partner)

    def relay(i):
        for d in PEERS:
            gather(i, d).wait_recv()
            forward(i, d).start()

    def step_body(j, carry):
        for i in range(NCHUNK):
            flat = advance(i).astype(BF16).T
            for q in range(HALF):
                u[i, pl.ds(pl.multiple_of(COLS * chip, 16), COLS),
                  pl.ds(pl.multiple_of(HALF * CHUNK * core + CHUNK * q, 128), CHUNK)] = flat[COLS * q:COLS * q + COLS, :]
            for d in PEERS:
                gather(i, d).start()
            forward(i, 0).start()
        kry_start(j - 1)
        sig[...] = jnp.zeros_like(sig)
        relay(0)

        def body(n, carry):
            i = lax.div(n, 2)
            g = 2 * lax.rem(n, 2)

            for c in range(NCHUNK):
                @pl.when(n == 2 * c)
                def _():
                    for d in range(8):
                        forward(c, d).wait_recv()
            for c in range(1, NCHUNK):
                @pl.when(n == 2 * c - 1)
                def _():
                    relay(c)

            right_part(i, g, ya)
            right_part(i, g + 1, yb)
            pair_part(i, g, ya, 0)
            left_part(i, g, 0)
            pair_part(i, g + 1, yb, 1)
            left_part(i, g + 1, 1)
            return carry

        lax.fori_loop(0, 6, body, 0)
        for i in range(NCHUNK):
            forward(i, 0).wait_send()
            for d in PEERS:
                gather(i, d).wait_send()
                forward(i, d).wait_send()
        kry_wait(j - 1)
        vector_part(j)
        return carry

    lax.fori_loop(1, STEPS, step_body, 0)
    for i in range(NCHUNK):
        advance(i)
    kry_start(STEPS - 1)
    kry_wait(STEPS - 1)


def run_steps(psi, left_loc, r_in, w_in):
    dma = pltpu.SemaphoreType.DMA
    vmem = pl.BlockSpec(memory_space=pltpu.VMEM)
    hbm = pl.BlockSpec(memory_space=pl.ANY)
    return pl.pallas_call(
        kernel,
        out_shape=(jax.ShapeDtypeStruct((STEPS, 16, ROWS, BOND), F32),
                   jax.ShapeDtypeStruct((STEPS, 8, 128), F32),
                   jax.ShapeDtypeStruct((STEPS, 8, 128), F32),
                   jax.ShapeDtypeStruct((ROWS * PAIR, BOND), F32)),
        in_specs=[hbm, hbm, hbm, vmem],
        out_specs=(hbm, vmem, vmem, vmem),
        scratch_shapes=[
            pltpu.VMEM((3, BOND * PAIR, 128), F32),
            pltpu.VMEM((NCHUNK, BOND, PAIR * CHUNK), BF16),
            pltpu.VMEM((NCHUNK, BOND, CHIPS * KLOC * CHUNK), BF16),
            pltpu.VMEM((CHIPS, KLOC, COLS, BOND), BF16),
            pltpu.VMEM((CHIPS, KLOC * 16, 128), BF16),
            pltpu.VMEM((CHIPS * KLOC, 256, 256), BF16),
            pltpu.VMEM((2 * KLOC * COLS, PAIR * CHUNK), BF16),
            pltpu.VMEM((2 * KLOC * COLS, PAIR * CHUNK), BF16),
            pltpu.VMEM((12, PAIR * COLS, 2 * KLOC * CHUNK), BF16),
            pltpu.VMEM((BOND, PAIR * COLS), F32),
            pltpu.VMEM((BOND, QROWS), F32),
            pltpu.VMEM((BOND, QROWS), F32),
            pltpu.VMEM((BOND, QROWS), F32),
            pltpu.VMEM((BOND, QROWS), F32),
            pltpu.VMEM((2, 16 * 8, 128), F32),
            pltpu.VMEM((8, 128), F32),
            pltpu.VMEM((8, 128), F32),
            pltpu.VMEM((8, 128), F32),
            dma((4, 3)), dma((NCHUNK, KLOC)), dma, dma((8,)), dma((8,)), dma((8,)), dma((8,)),
            dma((NCHUNK, 4, 2)), dma((NCHUNK, 4, 2)),
            dma((NCHUNK, 8)), dma((NCHUNK, 8)), dma((NCHUNK, 8)), dma((NCHUNK, 8)),
            dma, dma, dma((2, 16)), dma((2, 16)), dma((16,)), dma((16,)), dma,
        ],
        compiler_params=pltpu.CompilerParams(collective_id=0, has_side_effects=True, vmem_limit_bytes=60 * 1024 * 1024),
        name='lanczos',
    )(psi, left_loc, r_in, w_in)


def place_kernel(first_ref, block_ref, out_ref):
    j = pl.program_id(0)

    @pl.when(j == 0)
    def _():
        out_ref[0] = first_ref[...]

    @pl.when(j > 0)
    def _():
        for h in range(2):
            for q in range(HALF):
                pieces = [block_ref[0, 2 * c + h, :, COLS * q:COLS * q + COLS] for c in range(CHIPS)]
                out_ref[0, :, HALF * h + q, :] = jnp.concatenate(pieces, axis=1)


def place_rows(first, blocks):
    return pl.pallas_call(
        place_kernel,
        grid=(STEPS + 1,),
        out_shape=jax.ShapeDtypeStruct((STEPS + 1, ROWS, PAIR, BOND), F32),
        in_specs=[pl.BlockSpec((ROWS, PAIR, BOND), lambda j: (0, 0, 0)),
                  pl.BlockSpec((1, 16, ROWS, BOND), lambda j: (jnp.maximum(j - 1, 0), 0, 0, 0))],
        out_specs=pl.BlockSpec((1, ROWS, PAIR, BOND), lambda j: (j, 0, 0, 0)),
        name='place_rows',
    )(first, blocks)


def solution(mesh):
    def device_body(psi, left_loc, pair_loc, right_loc, flag_loc):
        r_in = jnp.where((flag_loc == 1)[:, None, None], right_loc, jnp.eye(BOND, dtype=BF16))
        w_in = jnp.pad(pair_loc.reshape(KLOC * PAIR, PAIR), ((0, 0), (0, 128 - PAIR)))
        blocks, alpha, beta, first = run_steps(psi.reshape(BOND * PAIR, BOND), left_loc, r_in, w_in)
        krylov = place_rows(first.reshape(ROWS, PAIR, BOND), blocks)
        return krylov, alpha[:, 0, 0], beta[:, 0, 0]

    return jax.shard_map(device_body, mesh=mesh, in_specs=(P(), P(AXIS), P(AXIS), P(AXIS), P(AXIS)),
                         out_specs=(P(None, AXIS), P(), P()), check_vma=False)
```

```python
import jax
import jax.numpy as jnp
from jax import lax
from jax.experimental import pallas as pl
from jax.experimental.pallas import tpu as pltpu
from jax.sharding import PartitionSpec as P

STEPS = 6
AXIS = 'terms'
BOND = 384
PAIR = 16
VEC_SIZE = BOND * PAIR * BOND
CHIPS = 8
COLS = BOND // CHIPS
HALF = PAIR // 2
KLOC = 4
CHUNK = 128
NCHUNK = BOND // CHUNK
QROWS = HALF * COLS
ROWS = BOND // 16
MESH = pl.DeviceIdType.MESH
F32 = jnp.float32
BF16 = jnp.bfloat16
PEERS = (1, 2, 4, 3, 5, 6, 7)
FORWARD_AT = 3


def flip(idx, mask, bits):
    out = 0
    for b in range(bits):
        bit = lax.rem(lax.div(idx, 1 << b), 2)
        if (mask >> b) & 1:
            bit = 1 - bit
        out = out + bit * (1 << b)
    return out


def rotl(pos, chunk):
    scaled = pos * (1 + chunk + lax.div(chunk, 2)) if not isinstance(chunk, int) else pos * (1 << chunk)
    return scaled - 7 * lax.div(scaled, 8)


def kernel(psi_ref, l_ref, r_ref, w_ref,
           kry_ref, alpha_ref, beta_ref, first_ref,
           psi, u, lbuf, rbuf, wbuf, mbuf, ya, yb, z, sig, sig_in, wv, vcur, vprev, red, norm_v, delta_now, beta_now,
           psi_sem, ll_sem, loc_sem, rs_sem, rr_sem, ws_sem, wr_sem, ls_sem, lr_sem, gs_sem, gr_sem, fs_sem, fr_sem,
           xs_sem, xr_sem, ds_sem, dr_sem, ks_sem, kr_sem, kl_sem):
    me = lax.axis_index(AXIS)
    chip = lax.div(me, 2)
    core = lax.rem(me, 2)
    partner = flip(me, 1, 4)

    def peer(d):
        return flip(chip, d, 3) * 2 + core

    def remote(src, dst, ssem, rsem, dev):
        return pltpu.make_async_remote_copy(src_ref=src, dst_ref=dst, send_sem=ssem, recv_sem=rsem,
                                            device_id=(dev,), device_id_type=MESH)

    l_own = [[pltpu.make_async_copy(l_ref.at[k, :, pl.ds(CHUNK * i, CHUNK)], lbuf.at[i, :, pl.ds(CHUNK * k, CHUNK)], ll_sem.at[i, k])
              for k in range(KLOC)] for i in range(NCHUNK)]
    r_own = pltpu.make_async_copy(r_ref.at[:, pl.ds(pl.multiple_of(COLS * chip, 16), COLS)], rbuf.at[0], loc_sem)
    part_rows = BOND * PAIR // 4
    psi_own = [[pltpu.make_async_copy(psi_ref.at[pl.ds(part_rows * i, part_rows), pl.ds(128 * c, 128)],
                                      psi.at[c, pl.ds(part_rows * i, part_rows)], psi_sem.at[i, c]) for c in range(3)]
               for i in range(4)]
    for i in range(NCHUNK):
        for k in range(KLOC):
            l_own[i][k].start()
    r_own.start()
    for i in range(4):
        for c in range(3):
            psi_own[i][c].start()
    barrier = pltpu.get_barrier_semaphore()
    for d in range(1, 16):
        pl.semaphore_signal(barrier, inc=1, device_id=(flip(me, d, 4),), device_id_type=MESH)
    pl.semaphore_wait(barrier, 15)

    w_copies = {d: remote(w_ref, wbuf.at[d], ws_sem.at[d], wr_sem.at[d], peer(d)) for d in PEERS}
    r_copies = {d: remote(r_ref.at[:, pl.ds(pl.multiple_of(COLS * flip(chip, d, 3), 16), COLS)], rbuf.at[d],
                          rs_sem.at[d], rr_sem.at[d], peer(d)) for d in PEERS}

    def l_copies(i, n):
        mask = 1 << ((i + min(n, 2)) % 3)
        src, dst, size = ((0, 512, 512), (0, 1024, 1024), (0, 2048, 1024), (1024, 3072, 1024))[n]
        spans = ((CHUNK * i, 2 * CHUNK),) if i < 2 else ((2 * CHUNK, CHUNK), (0, CHUNK))
        return [remote(lbuf.at[i, pl.ds(row, num), pl.ds(src, size)], lbuf.at[i, pl.ds(row, num), pl.ds(dst, size)],
                       ls_sem.at[i, n, m], lr_sem.at[i, n, m], peer(mask)) for m, (row, num) in enumerate(spans)]

    def l_start(i, n):
        for c in l_copies(i, n):
            c.start()

    def l_wait(i, n):
        for c in l_copies(i, n):
            c.wait_recv()

    for d in PEERS:
        w_copies[d].start()
    for d in (1, 2, 4):
        r_copies[d].start()
    for i in range(NCHUNK):
        for k in range(KLOC):
            l_own[i][k].wait()
        l_start(i, 0)
    for d in (3, 5, 6, 7):
        r_copies[d].start()

    wbuf[0] = w_ref[...]
    for d in PEERS:
        w_copies[d].wait_recv()
    row_id = lax.broadcasted_iota(jnp.int32, (256, 16), 0)
    col_id = lax.broadcasted_iota(jnp.int32, (256, 16), 1)
    spread = jnp.where(lax.div(row_id, 16) == col_id, 1.0, 0.0).astype(BF16)
    row_id = lax.broadcasted_iota(jnp.int32, (128, 256), 0)
    col_id = lax.broadcasted_iota(jnp.int32, (128, 256), 1)
    spread_t = jnp.where(row_id == lax.div(col_id, 16), 1.0, 0.0).astype(BF16)
    row_id = lax.broadcasted_iota(jnp.int32, (256, 256), 0)
    col_id = lax.broadcasted_iota(jnp.int32, (256, 256), 1)
    same = lax.rem(row_id, 16) == lax.rem(col_id, 16)

    def build(slot, carry):
        for k in range(KLOC):
            tall = jnp.dot(spread, wbuf[slot, pl.ds(16 * k, 16), :], preferred_element_type=F32).astype(BF16)
            full = jnp.dot(tall, spread_t, preferred_element_type=F32)
            mbuf[slot * KLOC + k] = jnp.where(same, full, 0.0).astype(BF16)
        return carry

    lax.fori_loop(0, CHIPS, build, 0)

    def right_part(i, g, y):
        slot_a = rotl(2 * g, i)
        slot_b = rotl(2 * g + 1, i)
        right = jnp.concatenate([rbuf[slot_a].reshape(KLOC * COLS, BOND), rbuf[slot_b].reshape(KLOC * COLS, BOND)], axis=0)
        for n in range(8):
            lanes = pl.ds(256 * n, 256)
            y[:, lanes] = jnp.dot(right, u[i, :, lanes], preferred_element_type=F32).astype(BF16)

    def pair_part(i, g, y, slot):
        slot_a = rotl(2 * g, i)
        slot_b = rotl(2 * g + 1, i)
        for kk in range(8):
            mat = mbuf[(slot_a if kk < KLOC else slot_b) * KLOC + kk % KLOC]
            cols = [jnp.concatenate([y[COLS * kk + 16 * t:COLS * kk + 16 * t + 16, 128 * r:128 * r + 128]
                                     for r in range(PAIR)], axis=0) for t in range(3)]
            pair = jnp.dot(mat, jnp.concatenate(cols, axis=1), preferred_element_type=F32).astype(BF16)
            for q in range(PAIR):
                for t in range(3):
                    z[slot, COLS * q + 16 * t:COLS * q + 16 * t + 16, 128 * kk:128 * kk + 128] = \
                        pair[16 * q:16 * q + 16, 128 * t:128 * t + 128]

    def left_part(i, g, slot):
        left = lbuf[i, :, pl.ds(pl.multiple_of(g * 1024, 1024), 1024)]
        sig[...] += lax.dot_general(left, z[slot], (((1,), (1,)), ((), ())), preferred_element_type=F32)

    def fold(x):
        out = x[0:8, 0:128]
        for r in range(COLS // 8):
            for c in range(NCHUNK):
                if r or c:
                    out = out + x[8 * r:8 * r + 8, 128 * c:128 * c + 128]
        return out

    def total(x):
        return jnp.sum(x, keepdims=True)

    def vector_part(j):
        lanes = pl.ds(pl.multiple_of(QROWS * core, 128), QROWS)
        swap = remote(sig.at[:, pl.ds(pl.multiple_of(QROWS * (1 - core), 128), QROWS)], sig_in, xs_sem, xr_sem, partner)
        swap.start()
        beta_old = beta_now[0:1, 0:1]
        swap.wait_recv()
        s_wv = jnp.zeros((8, 128), F32)
        s_cv = jnp.zeros((8, 128), F32)
        for n in range(BOND // COLS):
            rows = pl.ds(COLS * n, COLS)
            w = sig[rows, lanes] + sig_in[rows, :]
            v = vcur[rows, :]
            s_wv = s_wv + fold(w * v)
            w = w - beta_old * vprev[rows, :]
            s_cv = s_cv + fold(w * v)
            wv[rows, :] = w
        s_vv = total(norm_v[...])
        guess = jnp.where(s_vv > 0.0, total(s_cv) / jnp.where(s_vv > 0.0, s_vv, 1.0), 0.0)
        s_ww = jnp.zeros((8, 128), F32)
        s_w2v = jnp.zeros((8, 128), F32)
        for n in range(BOND // COLS):
            rows = pl.ds(COLS * n, COLS)
            v = vcur[rows, :]
            w = wv[rows, :] - guess * v
            wv[rows, :] = w
            s_ww = s_ww + fold(w * w)
            s_w2v = s_w2v + fold(w * v)
        row_of = lax.broadcasted_iota(jnp.int32, (8, 128), 0)
        message = jnp.where(row_of == 0, total(s_wv),
                            jnp.where(row_of == 1, guess,
                                      jnp.where(row_of == 2, s_vv, jnp.where(row_of == 3, total(s_ww), total(s_w2v)))))
        phase = lax.rem(j, 2)
        mine = pl.ds(pl.multiple_of(8 * me, 8), 8)
        red[phase, mine, :] = message
        copies = [remote(red.at[phase, mine], red.at[phase, mine], ds_sem.at[phase, d], dr_sem.at[phase, d], flip(me, d, 4))
                  for d in range(1, 16)]
        for c in copies:
            c.start()
        for c in copies:
            c.wait_recv()
        table = red.at[phase]
        a_wv, a_guess, a_vv, a_ww, a_w2v = [table[pl.ds(r, 16, stride=8), :] for r in range(5)]
        alpha = jnp.sum(a_wv, axis=0, keepdims=True) / VEC_SIZE
        shift = alpha - a_guess
        beta = jnp.sqrt(jnp.sum(a_ww - 2.0 * shift * a_w2v + shift * shift * a_vv, axis=0, keepdims=True) / VEC_SIZE)
        beta_now[...] = jnp.broadcast_to(beta, (8, 128))
        delta_now[...] = jnp.broadcast_to(alpha[0:1, 0:1] - guess, (8, 128))
        alpha_ref[j] = jnp.broadcast_to(alpha, (8, 128))
        beta_ref[j] = jnp.broadcast_to(beta, (8, 128))
        norm_v[...] = jnp.zeros_like(norm_v)
        for c in copies:
            c.wait_send()
        swap.wait_send()

    def advance(i):
        beta = beta_now[0:1, 0:1]
        delta = delta_now[0:1, 0:1]
        rows = pl.ds(CHUNK * i, CHUNK)
        old = vcur[rows, :]
        new = (wv[rows, :] - delta * old) / beta
        vprev[rows, :] = old
        vcur[rows, :] = new
        square = new * new
        acc = norm_v[...]
        for r in range(CHUNK // 8):
            for c in range(NCHUNK):
                acc = acc + square[8 * r:8 * r + 8, 128 * c:128 * c + 128]
        norm_v[...] = acc
        return new

    def kry_copies(j):
        return [remote(vcur.at[pl.ds(pl.multiple_of(ROWS * flip(me, d, 4), 8), ROWS)], kry_ref.at[j, me],
                       ks_sem.at[d], kr_sem.at[d], flip(me, d, 4)) for d in range(1, 16)]

    def kry_own(j):
        return pltpu.make_async_copy(vcur.at[pl.ds(pl.multiple_of(ROWS * me, 8), ROWS)], kry_ref.at[j, me], kl_sem)

    def kry_start(j):
        kry_own(j).start()
        for c in kry_copies(j):
            c.start()

    def kry_wait(j):
        kry_own(j).wait()
        for c in kry_copies(j):
            c.wait()

    square = jnp.zeros((8, 128), F32)
    for i in range(4):
        for c in range(3):
            psi_own[i][c].wait()

        def add_squares(n, acc, base=i * part_rows):
            for c in range(3):
                x = psi[c, pl.ds(pl.multiple_of(base + COLS * n, COLS), COLS), :]
                x = x * x
                for r in range(COLS // 8):
                    acc = acc + x[8 * r:8 * r + 8, :]
            return acc

        square = lax.fori_loop(0, part_rows // COLS, add_squares, square)
    norm = jnp.sqrt(jnp.sum(square, keepdims=True) / VEC_SIZE)

    def spread_pair(q, carry):
        for i in range(NCHUNK):
            for c in range(NCHUNK):
                x = psi[c, pl.ds(CHUNK * PAIR * i + q, CHUNK, stride=PAIR), :]
                x = (x / norm).T
                u[i, pl.ds(128 * c, 128), pl.ds(pl.multiple_of(CHUNK * q, CHUNK), CHUNK)] = x.astype(BF16)
                wv[pl.ds(128 * c, 128), pl.ds(CHUNK * i, CHUNK)] = x

        @pl.when(lax.div(q, HALF) == core)
        def _():
            sig[pl.ds(pl.multiple_of(COLS * lax.rem(q, HALF), COLS), COLS), 0:BOND] = wv[pl.ds(pl.multiple_of(COLS * chip, COLS), COLS), :]

        return carry

    lax.fori_loop(0, PAIR, spread_pair, 0)
    start = jnp.zeros((8, 128), F32)
    for i in range(NCHUNK):
        x = sig[:, pl.ds(CHUNK * i, CHUNK)].T
        vcur[pl.ds(CHUNK * i, CHUNK), :] = x
        x = x * x
        for r in range(CHUNK // 8):
            for c in range(NCHUNK):
                start = start + x[8 * r:8 * r + 8, 128 * c:128 * c + 128]
    norm_v[...] = start

    def first_rows(n, carry):
        for c in range(3):
            first_ref[pl.ds(pl.multiple_of(COLS * n, COLS), COLS), pl.ds(128 * c, 128)] = \
                psi[c, pl.ds(pl.multiple_of(ROWS * PAIR * me + COLS * n, COLS), COLS), :] / norm
        return carry

    lax.fori_loop(0, ROWS * PAIR // COLS, first_rows, 0)

    vprev[...] = jnp.zeros_like(vprev)
    beta_now[...] = jnp.zeros_like(beta_now)
    sig[...] = jnp.zeros_like(sig)
    r_own.wait()
    for i in range(NCHUNK):
        l_wait(i, 0)
        l_start(i, 1)
    for d in PEERS:
        r_copies[d].wait_recv()

    def front_body(n, carry):
        @pl.when(n == FORWARD_AT)
        def _():
            for i in range(NCHUNK):
                l_wait(i, 1)
                l_start(i, 2)
            for i in range(NCHUNK):
                l_start(i, 3)

        i = lax.div(n, 2)
        g = 2 * lax.rem(n, 2)
        right_part(i, g, ya)
        right_part(i, g + 1, yb)
        pair_part(i, g, ya, 4 * i + g)
        pair_part(i, g + 1, yb, 4 * i + g + 1)
        return carry

    lax.fori_loop(0, 6, front_body, 0)

    def mirror(i, g):
        other = lax.rem(i + 2, 3)
        for k in range(2):
            slot = rotl(2 * g + k, i)
            pos = rotl(slot, lax.rem(3 - other, 3))
            for n in range(KLOC):
                block = lbuf[other, pl.ds(pl.multiple_of(CHUNK * i, CHUNK), CHUNK),
                             pl.ds(pl.multiple_of(CHUNK * (KLOC * pos + n), CHUNK), CHUNK)]
                lbuf[i, pl.ds(pl.multiple_of(CHUNK * other, CHUNK), CHUNK),
                     pl.ds(pl.multiple_of(CHUNK * (KLOC * (2 * g + k) + n), CHUNK), CHUNK)] = block.T

    def back(g):
        def body(i, carry):
            mirror(i, g)
            left_part(i, g, 4 * i + g)
            return carry

        lax.fori_loop(0, NCHUNK, body, 0)

    back(0)
    for i in range(NCHUNK):
        l_wait(i, 2)
    back(2)
    for i in range(NCHUNK):
        l_wait(i, 3)
    back(1)
    back(3)
    for d in PEERS:
        w_copies[d].wait_send()
        r_copies[d].wait_send()
    for i in range(NCHUNK):
        for n in range(4):
            for c in l_copies(i, n):
                c.wait_send()
    vector_part(0)

    def region(i, c, r):
        return u.at[i, pl.ds(pl.multiple_of(COLS * c + 16 * r, 16), 16), pl.ds(pl.multiple_of(HALF * CHUNK * core, 1024), HALF * CHUNK)]

    def axis_of(r, ph):
        return 1 << ((r + ph) % 3)

    def masks(r, ph):
        out = [0]
        for n in range(ph):
            out += [m ^ axis_of(r, n) for m in out]
        return out

    def tree(i, ph, r):
        out = []
        for n, m in enumerate(masks(r, ph)):
            src = region(i, flip(chip, m, 3), r)
            num = (1 << ph) - 1 + n
            out.append(remote(src, src, gs_sem.at[i, r, num], gr_sem.at[i, r, num], peer(axis_of(r, ph))))
        return out

    def forward(i, r, m):
        src = region(i, flip(chip, m, 3), r)
        return remote(src, src, fs_sem.at[i, r, m], fr_sem.at[i, r, m], partner)

    def tree_start(i, ph):
        for r in range(3):
            for c in tree(i, ph, r):
                c.start()

    def tree_next(i, ph):
        for r in range(3):
            for c in tree(i, ph, r):
                c.wait_recv()
            if ph < 2:
                for c in tree(i, ph + 1, r):
                    c.start()
            for m in masks(r, ph):
                forward(i, r, m ^ axis_of(r, ph)).start()

    def step_body(j, carry):
        for i in range(NCHUNK):
            flat = advance(i).astype(BF16).T
            for q in range(HALF):
                u[i, pl.ds(pl.multiple_of(COLS * chip, 16), COLS),
                  pl.ds(pl.multiple_of(HALF * CHUNK * core + CHUNK * q, 128), CHUNK)] = flat[COLS * q:COLS * q + COLS, :]
            tree_start(i, 0)
            for r in range(3):
                forward(i, r, 0).start()
        sig[...] = jnp.zeros_like(sig)
        tree_next(0, 0)
        tree_next(1, 0)
        tree_next(0, 1)
        tree_next(1, 1)
        tree_next(2, 0)
        tree_next(0, 2)

        def body(n, carry):
            i = lax.div(n, 2)
            g = 2 * lax.rem(n, 2)

            @pl.when(n == 1)
            def _():
                tree_next(2, 1)
                tree_next(1, 2)
                kry_start(j - 1)

            @pl.when(n == 3)
            def _():
                tree_next(2, 2)

            for c in range(NCHUNK):
                @pl.when(n == 2 * c)
                def _():
                    for r in range(3):
                        for m in range(8):
                            forward(c, r, m).wait_recv()

            right_part(i, g, ya)
            right_part(i, g + 1, yb)
            pair_part(i, g, ya, 0)
            left_part(i, g, 0)
            pair_part(i, g + 1, yb, 1)
            left_part(i, g + 1, 1)
            return carry

        lax.fori_loop(0, 6, body, 0)
        for i in range(NCHUNK):
            for r in range(3):
                for m in range(8):
                    forward(i, r, m).wait_send()
                for ph in range(3):
                    for c in tree(i, ph, r):
                        c.wait_send()
        kry_wait(j - 1)
        vector_part(j)
        return carry

    lax.fori_loop(1, STEPS, step_body, 0)
    for i in range(NCHUNK):
        advance(i)
    kry_start(STEPS - 1)
    kry_wait(STEPS - 1)


def run_steps(psi, left_loc, r_in, w_in):
    dma = pltpu.SemaphoreType.DMA
    vmem = pl.BlockSpec(memory_space=pltpu.VMEM)
    hbm = pl.BlockSpec(memory_space=pl.ANY)
    return pl.pallas_call(
        kernel,
        out_shape=(jax.ShapeDtypeStruct((STEPS, 16, ROWS, BOND), F32),
                   jax.ShapeDtypeStruct((STEPS, 8, 128), F32),
                   jax.ShapeDtypeStruct((STEPS, 8, 128), F32),
                   jax.ShapeDtypeStruct((ROWS * PAIR, BOND), F32)),
        in_specs=[hbm, hbm, hbm, vmem],
        out_specs=(hbm, vmem, vmem, vmem),
        scratch_shapes=[
            pltpu.VMEM((3, BOND * PAIR, 128), F32),
            pltpu.VMEM((NCHUNK, BOND, PAIR * CHUNK), BF16),
            pltpu.VMEM((NCHUNK, BOND, CHIPS * KLOC * CHUNK), BF16),
            pltpu.VMEM((CHIPS, KLOC, COLS, BOND), BF16),
            pltpu.VMEM((CHIPS, KLOC * 16, 128), BF16),
            pltpu.VMEM((CHIPS * KLOC, 256, 256), BF16),
            pltpu.VMEM((2 * KLOC * COLS, PAIR * CHUNK), BF16),
            pltpu.VMEM((2 * KLOC * COLS, PAIR * CHUNK), BF16),
            pltpu.VMEM((12, PAIR * COLS, 2 * KLOC * CHUNK), BF16),
            pltpu.VMEM((BOND, PAIR * COLS), F32),
            pltpu.VMEM((BOND, QROWS), F32),
            pltpu.VMEM((BOND, QROWS), F32),
            pltpu.VMEM((BOND, QROWS), F32),
            pltpu.VMEM((BOND, QROWS), F32),
            pltpu.VMEM((2, 16 * 8, 128), F32),
            pltpu.VMEM((8, 128), F32),
            pltpu.VMEM((8, 128), F32),
            pltpu.VMEM((8, 128), F32),
            dma((4, 3)), dma((NCHUNK, KLOC)), dma, dma((8,)), dma((8,)), dma((8,)), dma((8,)),
            dma((NCHUNK, 4, 2)), dma((NCHUNK, 4, 2)),
            dma((NCHUNK, 3, 7)), dma((NCHUNK, 3, 7)), dma((NCHUNK, 3, 8)), dma((NCHUNK, 3, 8)),
            dma, dma, dma((2, 16)), dma((2, 16)), dma((16,)), dma((16,)), dma,
        ],
        compiler_params=pltpu.CompilerParams(collective_id=0, has_side_effects=True, vmem_limit_bytes=60 * 1024 * 1024),
        name='lanczos',
    )(psi, left_loc, r_in, w_in)


def place_kernel(first_ref, block_ref, out_ref):
    j = pl.program_id(0)

    @pl.when(j == 0)
    def _():
        out_ref[0] = first_ref[...]

    @pl.when(j > 0)
    def _():
        for h in range(2):
            for q in range(HALF):
                pieces = [block_ref[0, 2 * c + h, :, COLS * q:COLS * q + COLS] for c in range(CHIPS)]
                out_ref[0, :, HALF * h + q, :] = jnp.concatenate(pieces, axis=1)


def place_rows(first, blocks):
    return pl.pallas_call(
        place_kernel,
        grid=(STEPS + 1,),
        out_shape=jax.ShapeDtypeStruct((STEPS + 1, ROWS, PAIR, BOND), F32),
        in_specs=[pl.BlockSpec((ROWS, PAIR, BOND), lambda j: (0, 0, 0)),
                  pl.BlockSpec((1, 16, ROWS, BOND), lambda j: (jnp.maximum(j - 1, 0), 0, 0, 0))],
        out_specs=pl.BlockSpec((1, ROWS, PAIR, BOND), lambda j: (j, 0, 0, 0)),
        name='place_rows',
    )(first, blocks)


def solution(mesh):
    def device_body(psi, left_loc, pair_loc, right_loc, flag_loc):
        r_in = jnp.where((flag_loc == 1)[:, None, None], right_loc, jnp.eye(BOND, dtype=BF16))
        w_in = jnp.pad(pair_loc.reshape(KLOC * PAIR, PAIR), ((0, 0), (0, 128 - PAIR)))
        blocks, alpha, beta, first = run_steps(psi.reshape(BOND * PAIR, BOND), left_loc, r_in, w_in)
        krylov = place_rows(first.reshape(ROWS, PAIR, BOND), blocks)
        return krylov, alpha[:, 0, 0], beta[:, 0, 0]

    return jax.shard_map(device_body, mesh=mesh, in_specs=(P(), P(AXIS), P(AXIS), P(AXIS), P(AXIS)),
                         out_specs=(P(None, AXIS), P(), P()), check_vma=False)
```

```python
import jax
import jax.numpy as jnp
from jax import lax
from jax.experimental import pallas as pl
from jax.experimental.pallas import tpu as pltpu
from jax.sharding import PartitionSpec as P

STEPS = 6
AXIS = 'terms'
BOND = 384
PAIR = 16
VEC_SIZE = BOND * PAIR * BOND
CHIPS = 8
COLS = BOND // CHIPS
HALF = PAIR // 2
KLOC = 4
CHUNK = 128
NCHUNK = BOND // CHUNK
QROWS = HALF * COLS
ROWS = BOND // 16
MESH = pl.DeviceIdType.MESH
F32 = jnp.float32
BF16 = jnp.bfloat16
PEERS = (1, 2, 4, 3, 5, 6, 7)
FORWARD_AT = 3


def flip(idx, mask, bits):
    out = 0
    for b in range(bits):
        bit = lax.rem(lax.div(idx, 1 << b), 2)
        if (mask >> b) & 1:
            bit = 1 - bit
        out = out + bit * (1 << b)
    return out


def rotl(pos, chunk):
    scaled = pos * (1 + chunk + lax.div(chunk, 2)) if not isinstance(chunk, int) else pos * (1 << chunk)
    return scaled - 7 * lax.div(scaled, 8)


def kernel(psi_ref, l_ref, r_ref, w_ref, flag_ref,
           kry_ref, alpha_ref, beta_ref, first_ref,
           psi, u, lbuf, rsel, rbuf, wbuf, mbuf, ya, yb, z, sig, sig_in, wv, vcur, vprev, red, norm_v, delta_now, beta_now,
           psi_sem, ll_sem, loc_sem, rs_sem, rr_sem, ws_sem, wr_sem, ls_sem, lr_sem, gs_sem, gr_sem, fs_sem, fr_sem,
           xs_sem, xr_sem, ds_sem, dr_sem, ks_sem, kr_sem, kl_sem):
    me = lax.axis_index(AXIS)
    chip = lax.div(me, 2)
    core = lax.rem(me, 2)
    partner = flip(me, 1, 4)

    def peer(d):
        return flip(chip, d, 3) * 2 + core

    def remote(src, dst, ssem, rsem, dev):
        return pltpu.make_async_remote_copy(src_ref=src, dst_ref=dst, send_sem=ssem, recv_sem=rsem,
                                            device_id=(dev,), device_id_type=MESH)

    l_own = [[pltpu.make_async_copy(l_ref.at[k, :, pl.ds(CHUNK * i, CHUNK)], lbuf.at[i, :, pl.ds(CHUNK * k, CHUNK)], ll_sem.at[i, k])
              for k in range(KLOC)] for i in range(NCHUNK)]
    r_own = pltpu.make_async_copy(r_ref, rsel, loc_sem)
    part_rows = BOND * PAIR // 4
    psi_own = [[pltpu.make_async_copy(psi_ref.at[pl.ds(part_rows * i, part_rows), pl.ds(128 * c, 128)],
                                      psi.at[c, pl.ds(part_rows * i, part_rows)], psi_sem.at[i, c]) for c in range(3)]
               for i in range(4)]
    for i in range(NCHUNK):
        for k in range(KLOC):
            l_own[i][k].start()
    r_own.start()
    for i in range(4):
        for c in range(3):
            psi_own[i][c].start()
    barrier = pltpu.get_barrier_semaphore()
    for d in range(1, 16):
        pl.semaphore_signal(barrier, inc=1, device_id=(flip(me, d, 4),), device_id_type=MESH)
    pl.semaphore_wait(barrier, 15)

    w_copies = {d: remote(w_ref, wbuf.at[d], ws_sem.at[d], wr_sem.at[d], peer(d)) for d in PEERS}
    r_copies = {d: remote(rsel.at[:, pl.ds(pl.multiple_of(COLS * flip(chip, d, 3), 16), COLS)], rbuf.at[d],
                          rs_sem.at[d], rr_sem.at[d], peer(d)) for d in PEERS}

    def l_copies(i, n):
        mask = 1 << ((i + min(n, 2)) % 3)
        src, dst, size = ((0, 512, 512), (0, 1024, 1024), (0, 2048, 1024), (1024, 3072, 1024))[n]
        spans = ((CHUNK * i, 2 * CHUNK),) if i < 2 else ((2 * CHUNK, CHUNK), (0, CHUNK))
        return [remote(lbuf.at[i, pl.ds(row, num), pl.ds(src, size)], lbuf.at[i, pl.ds(row, num), pl.ds(dst, size)],
                       ls_sem.at[i, n, m], lr_sem.at[i, n, m], peer(mask)) for m, (row, num) in enumerate(spans)]

    def l_start(i, n):
        for c in l_copies(i, n):
            c.start()

    def l_wait(i, n):
        for c in l_copies(i, n):
            c.wait_recv()

    for d in PEERS:
        w_copies[d].start()
    for i in range(NCHUNK):
        for k in range(KLOC):
            l_own[i][k].wait()
        l_start(i, 0)

    r_own.wait()
    row_id = lax.broadcasted_iota(jnp.int32, (BOND, BOND), 0)
    col_id = lax.broadcasted_iota(jnp.int32, (BOND, BOND), 1)
    unit = jnp.where(row_id == col_id, 1.0, 0.0).astype(BF16)
    for k in range(KLOC):
        rsel[k] = jnp.where(jnp.full((BOND, BOND), flag_ref[k], jnp.int32) == 1, rsel[k].astype(F32), unit.astype(F32)).astype(BF16)
    for d in PEERS:
        r_copies[d].start()
    rbuf[0] = rsel[:, pl.ds(pl.multiple_of(COLS * chip, 16), COLS), :]

    wbuf[0] = w_ref[...]
    for d in PEERS:
        w_copies[d].wait_recv()
    row_id = lax.broadcasted_iota(jnp.int32, (256, 16), 0)
    col_id = lax.broadcasted_iota(jnp.int32, (256, 16), 1)
    spread = jnp.where(lax.div(row_id, 16) == col_id, 1.0, 0.0).astype(BF16)
    row_id = lax.broadcasted_iota(jnp.int32, (16, 256), 0)
    col_id = lax.broadcasted_iota(jnp.int32, (16, 256), 1)
    spread_t = jnp.where(row_id == lax.div(col_id, 16), 1.0, 0.0).astype(BF16)
    row_id = lax.broadcasted_iota(jnp.int32, (256, 256), 0)
    col_id = lax.broadcasted_iota(jnp.int32, (256, 256), 1)
    same = lax.rem(row_id, 16) == lax.rem(col_id, 16)

    def build(slot, carry):
        for k in range(KLOC):
            tall = jnp.dot(spread, wbuf[slot, pl.ds(16 * k, 16), :], preferred_element_type=F32).astype(BF16)
            full = jnp.dot(tall, spread_t, preferred_element_type=F32)
            mbuf[slot * KLOC + k] = jnp.where(same, full, 0.0).astype(BF16)
        return carry

    lax.fori_loop(0, CHIPS, build, 0)

    def right_part(i, g, y):
        slot_a = rotl(2 * g, i)
        slot_b = rotl(2 * g + 1, i)
        right = jnp.concatenate([rbuf[slot_a].reshape(KLOC * COLS, BOND), rbuf[slot_b].reshape(KLOC * COLS, BOND)], axis=0)
        for n in range(8):
            lanes = pl.ds(256 * n, 256)
            y[:, lanes] = jnp.dot(right, u[i, :, lanes], preferred_element_type=F32).astype(BF16)

    def pair_part(i, g, y, slot):
        slot_a = rotl(2 * g, i)
        slot_b = rotl(2 * g + 1, i)
        for kk in range(8):
            mat = mbuf[(slot_a if kk < KLOC else slot_b) * KLOC + kk % KLOC]
            cols = [jnp.concatenate([y[COLS * kk + 16 * t:COLS * kk + 16 * t + 16, 128 * r:128 * r + 128]
                                     for r in range(PAIR)], axis=0) for t in range(3)]
            pair = jnp.dot(mat, jnp.concatenate(cols, axis=1), preferred_element_type=F32).astype(BF16)
            for q in range(PAIR):
                for t in range(3):
                    z[slot, COLS * q + 16 * t:COLS * q + 16 * t + 16, 128 * kk:128 * kk + 128] = \
                        pair[16 * q:16 * q + 16, 128 * t:128 * t + 128]

    def left_part(i, g, slot):
        left = lbuf[i, :, pl.ds(pl.multiple_of(g * 1024, 1024), 1024)]
        sig[...] += lax.dot_general(left, z[slot], (((1,), (1,)), ((), ())), preferred_element_type=F32)

    def fold(x):
        out = x[0:8, 0:128]
        for r in range(COLS // 8):
            for c in range(NCHUNK):
                if r or c:
                    out = out + x[8 * r:8 * r + 8, 128 * c:128 * c + 128]
        return out

    def total(x):
        return jnp.sum(x, keepdims=True)

    def vector_part(j):
        lanes = pl.ds(pl.multiple_of(QROWS * core, 128), QROWS)
        other = pl.ds(pl.multiple_of(QROWS * (1 - core), 128), QROWS)
        swaps = [remote(sig.at[pl.ds(96 * n, 96), other], sig_in.at[pl.ds(96 * n, 96)], xs_sem.at[n], xr_sem.at[n], partner)
                 for n in range(4)]
        for c in swaps:
            c.start()
        beta_old = beta_now[0:1, 0:1]
        s_wv = jnp.zeros((8, 128), F32)
        s_cv = jnp.zeros((8, 128), F32)
        for n in range(BOND // COLS):
            if n % 2 == 0:
                swaps[n // 2].wait_recv()
            rows = pl.ds(COLS * n, COLS)
            w = sig[rows, lanes] + sig_in[rows, :]
            v = vcur[rows, :]
            s_wv = s_wv + fold(w * v)
            w = w - beta_old * vprev[rows, :]
            s_cv = s_cv + fold(w * v)
            wv[rows, :] = w
        s_vv = total(norm_v[...])
        guess = jnp.where(s_vv > 0.0, total(s_cv) / jnp.where(s_vv > 0.0, s_vv, 1.0), 0.0)
        s_ww = jnp.zeros((8, 128), F32)
        s_w2v = jnp.zeros((8, 128), F32)
        for n in range(BOND // COLS):
            rows = pl.ds(COLS * n, COLS)
            v = vcur[rows, :]
            w = wv[rows, :] - guess * v
            wv[rows, :] = w
            s_ww = s_ww + fold(w * w)
            s_w2v = s_w2v + fold(w * v)
        row_of = lax.broadcasted_iota(jnp.int32, (8, 128), 0)
        message = jnp.where(row_of == 0, total(s_wv),
                            jnp.where(row_of == 1, guess,
                                      jnp.where(row_of == 2, s_vv, jnp.where(row_of == 3, total(s_ww), total(s_w2v)))))
        phase = lax.rem(j, 2)
        mine = pl.ds(pl.multiple_of(8 * me, 8), 8)
        red[phase, mine, :] = message
        copies = [remote(red.at[phase, mine], red.at[phase, mine], ds_sem.at[phase, d], dr_sem.at[phase, d], flip(me, d, 4))
                  for d in range(1, 16)]
        for c in copies:
            c.start()
        for c in copies:
            c.wait_recv()
        table = red.at[phase]
        a_wv, a_guess, a_vv, a_ww, a_w2v = [table[pl.ds(r, 16, stride=8), :] for r in range(5)]
        alpha = jnp.sum(a_wv, axis=0, keepdims=True) / VEC_SIZE
        shift = alpha - a_guess
        beta = jnp.sqrt(jnp.sum(a_ww - 2.0 * shift * a_w2v + shift * shift * a_vv, axis=0, keepdims=True) / VEC_SIZE)
        beta_now[...] = jnp.broadcast_to(beta, (8, 128))
        delta_now[...] = jnp.broadcast_to(alpha[0:1, 0:1] - guess, (8, 128))
        alpha_ref[j] = jnp.broadcast_to(alpha, (8, 128))
        beta_ref[j] = jnp.broadcast_to(beta, (8, 128))
        norm_v[...] = jnp.zeros_like(norm_v)
        for c in copies:
            c.wait_send()
        for c in swaps:
            c.wait_send()

    def advance(i):
        beta = beta_now[0:1, 0:1]
        delta = delta_now[0:1, 0:1]
        rows = pl.ds(CHUNK * i, CHUNK)
        old = vcur[rows, :]
        new = (wv[rows, :] - delta * old) / beta
        vprev[rows, :] = old
        vcur[rows, :] = new
        square = new * new
        acc = norm_v[...]
        for r in range(CHUNK // 8):
            for c in range(NCHUNK):
                acc = acc + square[8 * r:8 * r + 8, 128 * c:128 * c + 128]
        norm_v[...] = acc
        return new

    def kry_copies(j):
        return [remote(vcur.at[pl.ds(pl.multiple_of(ROWS * flip(me, d, 4), 8), ROWS)], kry_ref.at[j, me],
                       ks_sem.at[d], kr_sem.at[d], flip(me, d, 4)) for d in range(1, 16)]

    def kry_own(j):
        return pltpu.make_async_copy(vcur.at[pl.ds(pl.multiple_of(ROWS * me, 8), ROWS)], kry_ref.at[j, me], kl_sem)

    def kry_start(j):
        kry_own(j).start()
        for c in kry_copies(j):
            c.start()

    def kry_wait(j):
        kry_own(j).wait()
        for c in kry_copies(j):
            c.wait()

    square = jnp.zeros((8, 128), F32)
    for i in range(4):
        for c in range(3):
            psi_own[i][c].wait()

        def add_squares(n, acc, base=i * part_rows):
            for c in range(3):
                x = psi[c, pl.ds(pl.multiple_of(base + COLS * n, COLS), COLS), :]
                x = x * x
                for r in range(COLS // 8):
                    acc = acc + x[8 * r:8 * r + 8, :]
            return acc

        square = lax.fori_loop(0, part_rows // COLS, add_squares, square)
    norm = jnp.sqrt(jnp.sum(square, keepdims=True) / VEC_SIZE)

    def spread_pair(q, carry):
        for i in range(NCHUNK):
            for c in range(NCHUNK):
                x = psi[c, pl.ds(CHUNK * PAIR * i + q, CHUNK, stride=PAIR), :]
                x = (x / norm).T
                u[i, pl.ds(128 * c, 128), pl.ds(pl.multiple_of(CHUNK * q, CHUNK), CHUNK)] = x.astype(BF16)
                wv[pl.ds(128 * c, 128), pl.ds(CHUNK * i, CHUNK)] = x

        @pl.when(lax.div(q, HALF) == core)
        def _():
            sig[pl.ds(pl.multiple_of(COLS * lax.rem(q, HALF), COLS), COLS), 0:BOND] = wv[pl.ds(pl.multiple_of(COLS * chip, COLS), COLS), :]

        return carry

    lax.fori_loop(0, PAIR, spread_pair, 0)
    start = jnp.zeros((8, 128), F32)
    for i in range(NCHUNK):
        x = sig[:, pl.ds(CHUNK * i, CHUNK)].T
        vcur[pl.ds(CHUNK * i, CHUNK), :] = x
        x = x * x
        for r in range(CHUNK // 8):
            for c in range(NCHUNK):
                start = start + x[8 * r:8 * r + 8, 128 * c:128 * c + 128]
    norm_v[...] = start

    def first_rows(n, carry):
        for c in range(3):
            first_ref[pl.ds(pl.multiple_of(COLS * n, COLS), COLS), pl.ds(128 * c, 128)] = \
                psi[c, pl.ds(pl.multiple_of(ROWS * PAIR * me + COLS * n, COLS), COLS), :] / norm
        return carry

    lax.fori_loop(0, ROWS * PAIR // COLS, first_rows, 0)

    vprev[...] = jnp.zeros_like(vprev)
    beta_now[...] = jnp.zeros_like(beta_now)
    sig[...] = jnp.zeros_like(sig)
    for i in range(NCHUNK):
        l_wait(i, 0)
        l_start(i, 1)
    for d in PEERS:
        r_copies[d].wait_recv()

    def front_body(n, carry):
        @pl.when(n == FORWARD_AT)
        def _():
            for i in range(NCHUNK):
                l_wait(i, 1)
                l_start(i, 2)
            for i in range(NCHUNK):
                l_start(i, 3)

        i = lax.div(n, 2)
        g = 2 * lax.rem(n, 2)
        right_part(i, g, ya)
        right_part(i, g + 1, yb)
        pair_part(i, g, ya, 4 * i + g)
        pair_part(i, g + 1, yb, 4 * i + g + 1)
        return carry

    lax.fori_loop(0, 6, front_body, 0)

    def mirror(i, g):
        other = lax.rem(i + 2, 3)
        for k in range(2):
            slot = rotl(2 * g + k, i)
            pos = rotl(slot, lax.rem(3 - other, 3))
            for n in range(KLOC):
                block = lbuf[other, pl.ds(pl.multiple_of(CHUNK * i, CHUNK), CHUNK),
                             pl.ds(pl.multiple_of(CHUNK * (KLOC * pos + n), CHUNK), CHUNK)]
                lbuf[i, pl.ds(pl.multiple_of(CHUNK * other, CHUNK), CHUNK),
                     pl.ds(pl.multiple_of(CHUNK * (KLOC * (2 * g + k) + n), CHUNK), CHUNK)] = block.T

    def back(g):
        def body(i, carry):
            mirror(i, g)
            left_part(i, g, 4 * i + g)
            return carry

        lax.fori_loop(0, NCHUNK, body, 0)

    back(0)
    for i in range(NCHUNK):
        l_wait(i, 2)
    back(2)
    for i in range(NCHUNK):
        l_wait(i, 3)
    back(1)
    back(3)
    for d in PEERS:
        w_copies[d].wait_send()
        r_copies[d].wait_send()
    for i in range(NCHUNK):
        for n in range(4):
            for c in l_copies(i, n):
                c.wait_send()
    vector_part(0)

    def region(i, c, r):
        return u.at[i, pl.ds(pl.multiple_of(COLS * c + 16 * r, 16), 16), pl.ds(pl.multiple_of(HALF * CHUNK * core, 1024), HALF * CHUNK)]

    def axis_of(r, ph):
        return 1 << ((r + ph) % 3)

    def masks(r, ph):
        out = [0]
        for n in range(ph):
            out += [m ^ axis_of(r, n) for m in out]
        return out

    def tree(i, ph, r):
        out = []
        for n, m in enumerate(masks(r, ph)):
            src = region(i, flip(chip, m, 3), r)
            num = (1 << ph) - 1 + n
            out.append(remote(src, src, gs_sem.at[i, r, num], gr_sem.at[i, r, num], peer(axis_of(r, ph))))
        return out

    def forward(i, r, m):
        src = region(i, flip(chip, m, 3), r)
        return remote(src, src, fs_sem.at[i, r, m], fr_sem.at[i, r, m], partner)

    def tree_start(i, ph):
        for r in range(3):
            for c in tree(i, ph, r):
                c.start()

    def tree_next(i, ph):
        for r in range(3):
            for c in tree(i, ph, r):
                c.wait_recv()
            if ph < 2:
                for c in tree(i, ph + 1, r):
                    c.start()
            for m in masks(r, ph):
                forward(i, r, m ^ axis_of(r, ph)).start()

    def step_body(j, carry):
        for i in range(NCHUNK):
            flat = advance(i).astype(BF16).T
            for q in range(HALF):
                u[i, pl.ds(pl.multiple_of(COLS * chip, 16), COLS),
                  pl.ds(pl.multiple_of(HALF * CHUNK * core + CHUNK * q, 128), CHUNK)] = flat[COLS * q:COLS * q + COLS, :]
            tree_start(i, 0)
            for r in range(3):
                forward(i, r, 0).start()
        sig[...] = jnp.zeros_like(sig)
        tree_next(0, 0)
        tree_next(1, 0)
        tree_next(0, 1)
        tree_next(1, 1)
        tree_next(2, 0)
        tree_next(0, 2)

        def body(n, carry):
            i = lax.div(n, 2)
            g = 2 * lax.rem(n, 2)

            @pl.when(n == 1)
            def _():
                tree_next(2, 1)
                tree_next(1, 2)
                kry_start(j - 1)

            @pl.when(n == 3)
            def _():
                tree_next(2, 2)

            for c in range(NCHUNK):
                @pl.when(n == 2 * c)
                def _():
                    for r in range(3):
                        for m in range(8):
                            forward(c, r, m).wait_recv()

            right_part(i, g, ya)
            right_part(i, g + 1, yb)
            pair_part(i, g, ya, 0)
            left_part(i, g, 0)
            pair_part(i, g + 1, yb, 1)
            left_part(i, g + 1, 1)
            return carry

        lax.fori_loop(0, 6, body, 0)
        for i in range(NCHUNK):
            for r in range(3):
                for m in range(8):
                    forward(i, r, m).wait_send()
                for ph in range(3):
                    for c in tree(i, ph, r):
                        c.wait_send()
        kry_wait(j - 1)
        vector_part(j)
        return carry

    lax.fori_loop(1, STEPS, step_body, 0)
    for i in range(NCHUNK):
        advance(i)
    kry_start(STEPS - 1)
    kry_wait(STEPS - 1)


def run_steps(psi, left_loc, right_loc, w_in, flag_loc):
    dma = pltpu.SemaphoreType.DMA
    vmem = pl.BlockSpec(memory_space=pltpu.VMEM)
    hbm = pl.BlockSpec(memory_space=pl.ANY)
    return pl.pallas_call(
        kernel,
        out_shape=(jax.ShapeDtypeStruct((STEPS, 16, ROWS, BOND), F32),
                   jax.ShapeDtypeStruct((STEPS, 8, 128), F32),
                   jax.ShapeDtypeStruct((STEPS, 8, 128), F32),
                   jax.ShapeDtypeStruct((ROWS * PAIR, BOND), F32)),
        in_specs=[hbm, hbm, hbm, vmem, pl.BlockSpec(memory_space=pltpu.SMEM)],
        out_specs=(hbm, vmem, vmem, vmem),
        scratch_shapes=[
            pltpu.VMEM((3, BOND * PAIR, 128), F32),
            pltpu.VMEM((NCHUNK, BOND, PAIR * CHUNK), BF16),
            pltpu.VMEM((NCHUNK, BOND, CHIPS * KLOC * CHUNK), BF16),
            pltpu.VMEM((KLOC, BOND, BOND), BF16),
            pltpu.VMEM((CHIPS, KLOC, COLS, BOND), BF16),
            pltpu.VMEM((CHIPS, KLOC * 16, PAIR), BF16),
            pltpu.VMEM((CHIPS * KLOC, 256, 256), BF16),
            pltpu.VMEM((2 * KLOC * COLS, PAIR * CHUNK), BF16),
            pltpu.VMEM((2 * KLOC * COLS, PAIR * CHUNK), BF16),
            pltpu.VMEM((12, PAIR * COLS, 2 * KLOC * CHUNK), BF16),
            pltpu.VMEM((BOND, PAIR * COLS), F32),
            pltpu.VMEM((BOND, QROWS), F32),
            pltpu.VMEM((BOND, QROWS), F32),
            pltpu.VMEM((BOND, QROWS), F32),
            pltpu.VMEM((BOND, QROWS), F32),
            pltpu.VMEM((2, 16 * 8, 128), F32),
            pltpu.VMEM((8, 128), F32),
            pltpu.VMEM((8, 128), F32),
            pltpu.VMEM((8, 128), F32),
            dma((4, 3)), dma((NCHUNK, KLOC)), dma, dma((8,)), dma((8,)), dma((8,)), dma((8,)),
            dma((NCHUNK, 4, 2)), dma((NCHUNK, 4, 2)),
            dma((NCHUNK, 3, 7)), dma((NCHUNK, 3, 7)), dma((NCHUNK, 3, 8)), dma((NCHUNK, 3, 8)),
            dma((4,)), dma((4,)), dma((2, 16)), dma((2, 16)), dma((16,)), dma((16,)), dma,
        ],
        compiler_params=pltpu.CompilerParams(collective_id=0, has_side_effects=True, vmem_limit_bytes=60 * 1024 * 1024),
        name='lanczos',
    )(psi, left_loc, right_loc, w_in, flag_loc)


def place_kernel(alpha_in, beta_in, first_ref, block_ref, out_ref, alpha_ref, beta_ref, tiles):
    j = pl.program_id(0)

    @pl.when(j == 0)
    def _():
        out_ref[0] = first_ref[...]
        for n in range(STEPS):
            alpha_ref[n] = alpha_in[n, 0, 0]
            beta_ref[n] = beta_in[n, 0, 0]

    @pl.when(j > 0)
    def _():
        for h in range(2):
            for q in range(HALF):
                row = jnp.concatenate([block_ref[0, 2 * c + h, :, COLS * q:COLS * q + COLS] for c in range(CHIPS)], axis=1)
                for n in range(ROWS // 8):
                    for t in range(3):
                        tiles[t, pl.ds(8 * PAIR * n + HALF * h + q, 8, stride=PAIR), :] = row[8 * n:8 * n + 8, 128 * t:128 * t + 128]
        for t in range(3):
            out_ref[0, :, 128 * t:128 * t + 128] = tiles[t]


def place_rows(alpha, beta, first, blocks):
    smem = pl.BlockSpec(memory_space=pltpu.SMEM)
    whole = pl.BlockSpec((STEPS, 8, 128), lambda j: (0, 0, 0))
    return pl.pallas_call(
        place_kernel,
        grid=(STEPS + 1,),
        out_shape=(jax.ShapeDtypeStruct((STEPS + 1, ROWS * PAIR, BOND), F32),
                   jax.ShapeDtypeStruct((STEPS,), F32), jax.ShapeDtypeStruct((STEPS,), F32)),
        in_specs=[whole, whole, pl.BlockSpec((ROWS * PAIR, BOND), lambda j: (0, 0)),
                  pl.BlockSpec((1, 16, ROWS, BOND), lambda j: (jnp.maximum(j - 1, 0), 0, 0, 0))],
        out_specs=(pl.BlockSpec((1, ROWS * PAIR, BOND), lambda j: (j, 0, 0)), smem, smem),
        scratch_shapes=[pltpu.VMEM((3, ROWS * PAIR, 128), F32)],
        name='place_rows',
    )(alpha, beta, first, blocks)


def solution(mesh):
    def device_body(psi, left_loc, pair_loc, right_loc, flag_loc):
        blocks, alpha, beta, first = run_steps(psi.reshape(BOND * PAIR, BOND), left_loc, right_loc,
                                               pair_loc.reshape(KLOC * PAIR, PAIR), flag_loc)
        krylov, alpha, beta = place_rows(alpha, beta, first, blocks)
        return krylov.reshape(STEPS + 1, ROWS, PAIR, BOND), alpha, beta

    return jax.shard_map(device_body, mesh=mesh, in_specs=(P(), P(AXIS), P(AXIS), P(AXIS), P(AXIS)),
                         out_specs=(P(None, AXIS), P(), P()), check_vma=False)
```

```python
import jax
import jax.numpy as jnp
from jax import lax
from jax.experimental import pallas as pl
from jax.experimental.pallas import tpu as pltpu
from jax.sharding import PartitionSpec as P

STEPS = 6
AXIS = 'terms'
BOND = 384
PAIR = 16
VEC_SIZE = BOND * PAIR * BOND
CHIPS = 8
COLS = BOND // CHIPS
HALF = PAIR // 2
KLOC = 4
CHUNK = 128
NCHUNK = BOND // CHUNK
QROWS = HALF * COLS
ROWS = BOND // 16
MESH = pl.DeviceIdType.MESH
F32 = jnp.float32
BF16 = jnp.bfloat16
PEERS = (1, 2, 4, 3, 5, 6, 7)
FORWARD_AT = 3


def flip(idx, mask, bits):
    out = 0
    for b in range(bits):
        bit = lax.rem(lax.div(idx, 1 << b), 2)
        if (mask >> b) & 1:
            bit = 1 - bit
        out = out + bit * (1 << b)
    return out


def rotl(pos, chunk):
    if isinstance(pos, int) and isinstance(chunk, int):
        return (pos << chunk) - 7 * ((pos << chunk) // 8)
    scaled = pos * (1 + chunk + lax.div(chunk, 2)) if not isinstance(chunk, int) else pos * (1 << chunk)
    return scaled - 7 * lax.div(scaled, 8)


def kernel(psi_ref, l_ref, r_ref, w_ref, flag_ref,
           kry_ref, alpha_ref, beta_ref, first_ref,
           psi, u, lbuf, rsel, rbuf, wbuf, mbuf, ya, yb, yc, yd, z, sig, sig_in, wv, vcur, vprev, red, norm_v, delta_now, beta_now,
           psi_sem, ll_sem, loc_sem, rs_sem, rr_sem, ws_sem, wr_sem, ls_sem, lr_sem, ns_sem, nr_sem, gs_sem, gr_sem, fs_sem, fr_sem,
           xs_sem, xr_sem, ds_sem, dr_sem, ks_sem, kr_sem, kl_sem):
    me = lax.axis_index(AXIS)
    chip = lax.div(me, 2)
    core = lax.rem(me, 2)
    partner = flip(me, 1, 4)

    def peer(d):
        return flip(chip, d, 3) * 2 + core

    def remote(src, dst, ssem, rsem, dev):
        return pltpu.make_async_remote_copy(src_ref=src, dst_ref=dst, send_sem=ssem, recv_sem=rsem,
                                            device_id=(dev,), device_id_type=MESH)

    l_own = [[pltpu.make_async_copy(l_ref.at[k, :, pl.ds(CHUNK * i, CHUNK)], lbuf.at[i, :, pl.ds(CHUNK * k, CHUNK)], ll_sem.at[i, k])
              for k in range(KLOC)] for i in range(NCHUNK)]
    r_own = pltpu.make_async_copy(r_ref, rsel, loc_sem)
    part_rows = BOND * PAIR // 4
    psi_own = [[pltpu.make_async_copy(psi_ref.at[pl.ds(part_rows * i, part_rows), pl.ds(128 * c, 128)],
                                      psi.at[c, pl.ds(part_rows * i, part_rows)], psi_sem.at[i, c]) for c in range(3)]
               for i in range(4)]
    for i in range(NCHUNK):
        for k in range(KLOC):
            l_own[i][k].start()
    r_own.start()
    for i in range(4):
        for c in range(3):
            psi_own[i][c].start()
    barrier = pltpu.get_barrier_semaphore()
    for d in range(1, 16):
        pl.semaphore_signal(barrier, inc=1, device_id=(flip(me, d, 4),), device_id_type=MESH)
    pl.semaphore_wait(barrier, 15)

    w_copies = {d: remote(w_ref, wbuf.at[d], ws_sem.at[d], wr_sem.at[d], peer(d)) for d in PEERS}
    r_copies = {d: remote(rsel.at[:, pl.ds(pl.multiple_of(COLS * flip(chip, d, 3), 16), COLS)], rbuf.at[d],
                          rs_sem.at[d], rr_sem.at[d], peer(d)) for d in PEERS}

    def l_copies(i, n):
        mask = 1 << ((i + min(n, 2)) % 3)
        src, dst, size = ((0, 512, 512), (0, 1024, 1024), (0, 2048, 1024), (1024, 3072, 1024))[n]
        spans = ((CHUNK * i, 2 * CHUNK),) if i < 2 else ((2 * CHUNK, CHUNK), (0, CHUNK))
        return [remote(lbuf.at[i, pl.ds(row, num), pl.ds(src, size)], lbuf.at[i, pl.ds(row, num), pl.ds(dst, size)],
                       ls_sem.at[i, n, m], lr_sem.at[i, n, m], peer(mask)) for m, (row, num) in enumerate(spans)]

    def l_start(i, n):
        for c in l_copies(i, n):
            c.start()

    def l_wait(i, n):
        for c in l_copies(i, n):
            c.wait_recv()

    for d in PEERS:
        w_copies[d].start()
    for i in range(NCHUNK):
        for k in range(KLOC):
            l_own[i][k].wait()
        l_start(i, 0)

    r_own.wait()
    row_id = lax.broadcasted_iota(jnp.int32, (BOND, BOND), 0)
    col_id = lax.broadcasted_iota(jnp.int32, (BOND, BOND), 1)
    unit = jnp.where(row_id == col_id, 1.0, 0.0).astype(BF16)
    for k in range(KLOC):
        rsel[k] = jnp.where(jnp.full((BOND, BOND), flag_ref[k], jnp.int32) == 1, rsel[k].astype(F32), unit.astype(F32)).astype(BF16)
    for d in PEERS:
        r_copies[d].start()
    rbuf[0] = rsel[:, pl.ds(pl.multiple_of(COLS * chip, 16), COLS), :]

    wbuf[0] = w_ref[...]
    for d in PEERS:
        w_copies[d].wait_recv()
    row_id = lax.broadcasted_iota(jnp.int32, (256, 16), 0)
    col_id = lax.broadcasted_iota(jnp.int32, (256, 16), 1)
    spread = jnp.where(lax.div(row_id, 16) == col_id, 1.0, 0.0).astype(BF16)
    row_id = lax.broadcasted_iota(jnp.int32, (16, 256), 0)
    col_id = lax.broadcasted_iota(jnp.int32, (16, 256), 1)
    spread_t = jnp.where(row_id == lax.div(col_id, 16), 1.0, 0.0).astype(BF16)
    row_id = lax.broadcasted_iota(jnp.int32, (256, 256), 0)
    col_id = lax.broadcasted_iota(jnp.int32, (256, 256), 1)
    same = lax.rem(row_id, 16) == lax.rem(col_id, 16)

    def build(slot, carry):
        for k in range(KLOC):
            tall = jnp.dot(spread, wbuf[slot, pl.ds(16 * k, 16), :], preferred_element_type=F32).astype(BF16)
            full = jnp.dot(tall, spread_t, preferred_element_type=F32)
            mbuf[slot * KLOC + k] = jnp.where(same, full, 0.0).astype(BF16)
        return carry

    lax.fori_loop(0, CHIPS, build, 0)

    def right_part(i, g, y, tiles=range(8)):
        slot_a = rotl(2 * g, i)
        slot_b = rotl(2 * g + 1, i)
        right = jnp.concatenate([rbuf[slot_a].reshape(KLOC * COLS, BOND), rbuf[slot_b].reshape(KLOC * COLS, BOND)], axis=0)
        for n in tiles:
            lanes = pl.ds(256 * n, 256)
            both = jnp.dot(right, u[i, :, lanes], preferred_element_type=F32).astype(BF16)
            y[2 * n] = both[:, 0:128]
            y[2 * n + 1] = both[:, 128:256]

    def pair_part(i, g, y, slot):
        slot_a = rotl(2 * g, i)
        slot_b = rotl(2 * g + 1, i)
        for kk in range(8):
            mat = mbuf[(slot_a if kk < KLOC else slot_b) * KLOC + kk % KLOC]
            cols = [y[:, pl.ds(COLS * kk + 16 * t, 16), :].reshape(PAIR * 16, CHUNK) for t in range(3)]
            pair = jnp.dot(mat, jnp.concatenate(cols, axis=1), preferred_element_type=F32).astype(BF16)
            for t in range(3):
                z[slot, :, pl.ds(16 * t, 16), pl.ds(128 * kk, 128)] = pair[:, 128 * t:128 * t + 128].reshape(PAIR, 16, CHUNK)

    def left_part(i, g, slot):
        left = lbuf[i, :, pl.ds(pl.multiple_of(g * 1024, 1024), 1024)]
        sig[...] += lax.dot_general(left, z[slot].reshape(PAIR * COLS, 2 * KLOC * CHUNK), (((1,), (1,)), ((), ())), preferred_element_type=F32)

    def fold(x):
        out = x[0:8, 0:128]
        for r in range(COLS // 8):
            for c in range(NCHUNK):
                if r or c:
                    out = out + x[8 * r:8 * r + 8, 128 * c:128 * c + 128]
        return out

    def total(x):
        return jnp.sum(x, keepdims=True)

    def vector_part(j):
        lanes = pl.ds(pl.multiple_of(QROWS * core, 128), QROWS)
        other = pl.ds(pl.multiple_of(QROWS * (1 - core), 128), QROWS)
        swaps = [remote(sig.at[pl.ds(96 * n, 96), other], sig_in.at[pl.ds(96 * n, 96)], xs_sem.at[n], xr_sem.at[n], partner)
                 for n in range(4)]
        for c in swaps:
            c.start()
        beta_old = beta_now[0:1, 0:1]
        s_wv = jnp.zeros((8, 128), F32)
        s_cv = jnp.zeros((8, 128), F32)
        for n in range(BOND // COLS):
            if n % 2 == 0:
                swaps[n // 2].wait_recv()
            rows = pl.ds(COLS * n, COLS)
            w = sig[rows, lanes] + sig_in[rows, :]
            v = vcur[rows, :]
            s_wv = s_wv + fold(w * v)
            w = w - beta_old * vprev[rows, :]
            s_cv = s_cv + fold(w * v)
            wv[rows, :] = w
        s_vv = total(norm_v[...])
        guess = jnp.where(s_vv > 0.0, total(s_cv) / jnp.where(s_vv > 0.0, s_vv, 1.0), 0.0)
        s_ww = jnp.zeros((8, 128), F32)
        s_w2v = jnp.zeros((8, 128), F32)
        for n in range(BOND // COLS):
            rows = pl.ds(COLS * n, COLS)
            v = vcur[rows, :]
            w = wv[rows, :] - guess * v
            wv[rows, :] = w
            s_ww = s_ww + fold(w * w)
            s_w2v = s_w2v + fold(w * v)
        row_of = lax.broadcasted_iota(jnp.int32, (8, 128), 0)
        message = jnp.where(row_of == 0, total(s_wv),
                            jnp.where(row_of == 1, guess,
                                      jnp.where(row_of == 2, s_vv, jnp.where(row_of == 3, total(s_ww), total(s_w2v)))))
        phase = lax.rem(j, 2)
        mine = pl.ds(pl.multiple_of(8 * me, 8), 8)
        red[phase, mine, :] = message
        copies = [remote(red.at[phase, mine], red.at[phase, mine], ds_sem.at[phase, d], dr_sem.at[phase, d], flip(me, d, 4))
                  for d in range(1, 16)]
        for c in copies:
            c.start()
        for c in copies:
            c.wait_recv()
        table = red.at[phase]
        a_wv, a_guess, a_vv, a_ww, a_w2v = [table[pl.ds(r, 16, stride=8), :] for r in range(5)]
        alpha = jnp.sum(a_wv, axis=0, keepdims=True) / VEC_SIZE
        shift = alpha - a_guess
        beta = jnp.sqrt(jnp.sum(a_ww - 2.0 * shift * a_w2v + shift * shift * a_vv, axis=0, keepdims=True) / VEC_SIZE)
        beta_now[...] = jnp.broadcast_to(beta, (8, 128))
        delta_now[...] = jnp.broadcast_to(alpha[0:1, 0:1] - guess, (8, 128))
        alpha_ref[j] = jnp.broadcast_to(alpha, (8, 128))
        beta_ref[j] = jnp.broadcast_to(beta, (8, 128))
        norm_v[...] = jnp.zeros_like(norm_v)
        for c in copies:
            c.wait_send()
        for c in swaps:
            c.wait_send()

    def advance(i):
        beta = beta_now[0:1, 0:1]
        delta = delta_now[0:1, 0:1]
        rows = pl.ds(CHUNK * i, CHUNK)
        old = vcur[rows, :]
        new = (wv[rows, :] - delta * old) / beta
        vprev[rows, :] = old
        vcur[rows, :] = new
        square = new * new
        acc = norm_v[...]
        for r in range(CHUNK // 8):
            for c in range(NCHUNK):
                acc = acc + square[8 * r:8 * r + 8, 128 * c:128 * c + 128]
        norm_v[...] = acc
        return new

    def kry_copies(j):
        return [remote(vcur.at[pl.ds(pl.multiple_of(ROWS * flip(me, d, 4), 8), ROWS)], kry_ref.at[j, me],
                       ks_sem.at[d], kr_sem.at[d], flip(me, d, 4)) for d in range(1, 16)]

    def kry_own(j):
        return pltpu.make_async_copy(vcur.at[pl.ds(pl.multiple_of(ROWS * me, 8), ROWS)], kry_ref.at[j, me], kl_sem)

    def kry_start(j):
        kry_own(j).start()
        for c in kry_copies(j):
            c.start()

    def kry_wait(j):
        kry_own(j).wait()
        for c in kry_copies(j):
            c.wait()

    square = jnp.zeros((8, 128), F32)
    for i in range(4):
        for c in range(3):
            psi_own[i][c].wait()

        def add_squares(n, acc, base=i * part_rows):
            for c in range(3):
                x = psi[c, pl.ds(pl.multiple_of(base + COLS * n, COLS), COLS), :]
                x = x * x
                for r in range(COLS // 8):
                    acc = acc + x[8 * r:8 * r + 8, :]
            return acc

        square = lax.fori_loop(0, part_rows // COLS, add_squares, square)
    norm = jnp.sqrt(jnp.sum(square, keepdims=True) / VEC_SIZE)

    def spread_pair(q, carry):
        for i in range(NCHUNK):
            for c in range(NCHUNK):
                x = psi[c, pl.ds(CHUNK * PAIR * i + q, CHUNK, stride=PAIR), :]
                x = (x / norm).T
                u[i, pl.ds(128 * c, 128), pl.ds(pl.multiple_of(CHUNK * q, CHUNK), CHUNK)] = x.astype(BF16)
                wv[pl.ds(128 * c, 128), pl.ds(CHUNK * i, CHUNK)] = x

        @pl.when(lax.div(q, HALF) == core)
        def _():
            sig[pl.ds(pl.multiple_of(COLS * lax.rem(q, HALF), COLS), COLS), 0:BOND] = wv[pl.ds(pl.multiple_of(COLS * chip, COLS), COLS), :]

        return carry

    lax.fori_loop(0, PAIR, spread_pair, 0)
    start = jnp.zeros((8, 128), F32)
    for i in range(NCHUNK):
        x = sig[:, pl.ds(CHUNK * i, CHUNK)].T
        vcur[pl.ds(CHUNK * i, CHUNK), :] = x
        x = x * x
        for r in range(CHUNK // 8):
            for c in range(NCHUNK):
                start = start + x[8 * r:8 * r + 8, 128 * c:128 * c + 128]
    norm_v[...] = start

    def first_rows(n, carry):
        for c in range(3):
            first_ref[pl.ds(pl.multiple_of(COLS * n, COLS), COLS), pl.ds(128 * c, 128)] = \
                psi[c, pl.ds(pl.multiple_of(ROWS * PAIR * me + COLS * n, COLS), COLS), :] / norm
        return carry

    lax.fori_loop(0, ROWS * PAIR // COLS, first_rows, 0)

    vprev[...] = jnp.zeros_like(vprev)
    beta_now[...] = jnp.zeros_like(beta_now)
    sig[...] = jnp.zeros_like(sig)
    for i in range(NCHUNK):
        l_wait(i, 0)
        l_start(i, 1)
    for d in PEERS:
        r_copies[d].wait_recv()

    def front_body(n, carry):
        @pl.when(n == FORWARD_AT)
        def _():
            for i in range(NCHUNK):
                l_wait(i, 1)
                l_start(i, 2)
            for i in range(NCHUNK):
                l_start(i, 3)

        i = lax.div(n, 2)
        g = 2 * lax.rem(n, 2)
        right_part(i, g, ya)
        right_part(i, g + 1, yb)
        pair_part(i, g, ya, 4 * i + g)
        pair_part(i, g + 1, yb, 4 * i + g + 1)
        return carry

    lax.fori_loop(0, 6, front_body, 0)

    def mirror(i, g):
        other = lax.rem(i + 2, 3)
        for k in range(2):
            slot = rotl(2 * g + k, i)
            pos = rotl(slot, lax.rem(3 - other, 3))
            for n in range(KLOC):
                block = lbuf[other, pl.ds(pl.multiple_of(CHUNK * i, CHUNK), CHUNK),
                             pl.ds(pl.multiple_of(CHUNK * (KLOC * pos + n), CHUNK), CHUNK)]
                lbuf[i, pl.ds(pl.multiple_of(CHUNK * other, CHUNK), CHUNK),
                     pl.ds(pl.multiple_of(CHUNK * (KLOC * (2 * g + k) + n), CHUNK), CHUNK)] = block.T

    def back(g):
        def body(i, carry):
            mirror(i, g)
            left_part(i, g, 4 * i + g)
            return carry

        lax.fori_loop(0, NCHUNK, body, 0)

    back(0)
    for i in range(NCHUNK):
        l_wait(i, 2)
    back(2)
    for i in range(NCHUNK):
        l_wait(i, 3)
    back(1)
    back(3)
    for d in PEERS:
        w_copies[d].wait_send()
        r_copies[d].wait_send()
    for i in range(NCHUNK):
        for n in range(4):
            for c in l_copies(i, n):
                c.wait_send()
    vector_part(0)

    units = ((0, 0, 512), (0, 512, 512), (1, 0, 1024), (2, 0, 1024))

    def region(un, mask, lo, width):
        i, first, _ = units[un]
        return u.at[i, pl.ds(pl.multiple_of(COLS * flip(chip, mask, 3), 16), COLS),
                    pl.ds(pl.multiple_of(HALF * CHUNK * core + first + lo, 128), width)]

    def near(un, a):
        own = region(un, 0, 0, units[un][2])
        return remote(own, own, ns_sem.at[un, a], nr_sem.at[un, a], peer(1 << a))

    def far(un):
        own = region(un, 0, 0, units[un][2])
        return remote(own, own, ns_sem.at[un, 3], nr_sem.at[un, 3], peer(7))

    def second(un, a, h):
        half = units[un][2] // 2
        block = region(un, 1 << a, half * h, half)
        return remote(block, block, gs_sem.at[un, 2 * a + h], gr_sem.at[un, 2 * a + h], peer(1 << ((a + 1 + h) % 3)))

    def cross(un, n):
        width = units[un][2]
        if n < 5:
            block = region(un, (0, 1, 2, 4, 7)[n], 0, width)
        else:
            a, h = divmod(n - 5, 2)
            block = region(un, (1 << a) ^ (1 << ((a + 1 + h) % 3)), width // 2 * h, width // 2)
        return remote(block, block, fs_sem.at[un, n], fr_sem.at[un, n], partner)

    def send_out(un):
        for a in range(3):
            near(un, a).start()
        far(un).start()
        cross(un, 0).start()

    def hop(un):
        for a in range(3):
            near(un, a).wait_recv()
            second(un, a, 0).start()
            second(un, a, 1).start()
            cross(un, 1 + a).start()

    def land(un):
        far(un).wait_recv()
        cross(un, 4).start()
        for a in range(3):
            for h in range(2):
                second(un, a, h).wait_recv()
                cross(un, 5 + 2 * a + h).start()

    def ready(un):
        for n in range(11):
            cross(un, n).wait_recv()

    def sent(un):
        for a in range(3):
            near(un, a).wait_send()
        far(un).wait_send()
        for a in range(3):
            for h in range(2):
                second(un, a, h).wait_send()
        for n in range(11):
            cross(un, n).wait_send()

    def publish(i):
        flat = advance(i).astype(BF16).T
        for q in range(HALF):
            u[i, pl.ds(pl.multiple_of(COLS * chip, 16), COLS),
              pl.ds(pl.multiple_of(HALF * CHUNK * core + CHUNK * q, 128), CHUNK)] = flat[COLS * q:COLS * q + COLS, :]

    def step_body(j, carry):
        publish(0)
        send_out(0)
        send_out(1)
        publish(1)
        publish(2)
        sig[...] = jnp.zeros_like(sig)
        hop(0)
        hop(1)
        send_out(2)
        land(0)
        ready(0)
        for g, y in enumerate((ya, yb, yc, yd)):
            right_part(0, g, y, (0, 1, 4, 5))
        land(1)
        ready(1)
        right_part(0, 0, ya, (2, 3, 6, 7))
        right_part(0, 1, yb, (2, 3, 6, 7))
        hop(2)
        send_out(3)
        pair_part(0, 0, ya, 0)
        left_part(0, 0, 0)
        pair_part(0, 1, yb, 1)
        left_part(0, 1, 1)
        right_part(0, 2, yc, (2, 3, 6, 7))
        right_part(0, 3, yd, (2, 3, 6, 7))
        pair_part(0, 2, yc, 0)
        left_part(0, 2, 0)
        land(2)
        pair_part(0, 3, yd, 1)
        left_part(0, 3, 1)
        ready(2)

        def body(n, carry):
            i = lax.div(n, 2)
            g = 2 * lax.rem(n, 2)

            @pl.when(n == 4)
            def _():
                ready(3)

            right_part(i, g, ya)
            right_part(i, g + 1, yb)

            pair_part(i, g, ya, 0)
            left_part(i, g, 0)

            @pl.when(n == 2)
            def _():
                hop(3)

            @pl.when(n == 3)
            def _():
                land(3)
                kry_start(j - 1)

            pair_part(i, g + 1, yb, 1)
            left_part(i, g + 1, 1)
            return carry

        lax.fori_loop(2, 6, body, 0)
        for un in range(4):
            sent(un)
        kry_wait(j - 1)
        vector_part(j)
        return carry

    lax.fori_loop(1, STEPS, step_body, 0)
    for i in range(NCHUNK):
        advance(i)
    kry_start(STEPS - 1)
    kry_wait(STEPS - 1)


def run_steps(psi, left_loc, right_loc, w_in, flag_loc):
    dma = pltpu.SemaphoreType.DMA
    vmem = pl.BlockSpec(memory_space=pltpu.VMEM)
    hbm = pl.BlockSpec(memory_space=pl.ANY)
    return pl.pallas_call(
        kernel,
        out_shape=(jax.ShapeDtypeStruct((STEPS, 16, ROWS, BOND), F32),
                   jax.ShapeDtypeStruct((STEPS, 8, 128), F32),
                   jax.ShapeDtypeStruct((STEPS, 8, 128), F32),
                   jax.ShapeDtypeStruct((ROWS * PAIR, BOND), F32)),
        in_specs=[hbm, hbm, hbm, vmem, pl.BlockSpec(memory_space=pltpu.SMEM)],
        out_specs=(hbm, vmem, vmem, vmem),
        scratch_shapes=[
            pltpu.VMEM((3, BOND * PAIR, 128), F32),
            pltpu.VMEM((NCHUNK, BOND, PAIR * CHUNK), BF16),
            pltpu.VMEM((NCHUNK, BOND, CHIPS * KLOC * CHUNK), BF16),
            pltpu.VMEM((KLOC, BOND, BOND), BF16),
            pltpu.VMEM((CHIPS, KLOC, COLS, BOND), BF16),
            pltpu.VMEM((CHIPS, KLOC * 16, PAIR), BF16),
            pltpu.VMEM((CHIPS * KLOC, 256, 256), BF16),
            pltpu.VMEM((PAIR, 2 * KLOC * COLS, CHUNK), BF16),
            pltpu.VMEM((PAIR, 2 * KLOC * COLS, CHUNK), BF16),
            pltpu.VMEM((PAIR, 2 * KLOC * COLS, CHUNK), BF16),
            pltpu.VMEM((PAIR, 2 * KLOC * COLS, CHUNK), BF16),
            pltpu.VMEM((12, PAIR, COLS, 2 * KLOC * CHUNK), BF16),
            pltpu.VMEM((BOND, PAIR * COLS), F32),
            pltpu.VMEM((BOND, QROWS), F32),
            pltpu.VMEM((BOND, QROWS), F32),
            pltpu.VMEM((BOND, QROWS), F32),
            pltpu.VMEM((BOND, QROWS), F32),
            pltpu.VMEM((2, 16 * 8, 128), F32),
            pltpu.VMEM((8, 128), F32),
            pltpu.VMEM((8, 128), F32),
            pltpu.VMEM((8, 128), F32),
            dma((4, 3)), dma((NCHUNK, KLOC)), dma, dma((8,)), dma((8,)), dma((8,)), dma((8,)),
            dma((NCHUNK, 4, 2)), dma((NCHUNK, 4, 2)),
            dma((4, 4)), dma((4, 4)), dma((4, 6)), dma((4, 6)), dma((4, 11)), dma((4, 11)),
            dma((4,)), dma((4,)), dma((2, 16)), dma((2, 16)), dma((16,)), dma((16,)), dma,
        ],
        compiler_params=pltpu.CompilerParams(collective_id=0, has_side_effects=True, vmem_limit_bytes=60 * 1024 * 1024),
        name='lanczos',
    )(psi, left_loc, right_loc, w_in, flag_loc)


def place_kernel(alpha_in, beta_in, first_ref, block_ref, out_ref, alpha_ref, beta_ref, tiles):
    j = pl.program_id(0)

    @pl.when(j == 0)
    def _():
        out_ref[0] = first_ref[...]
        for n in range(STEPS):
            alpha_ref[n] = alpha_in[n, 0, 0]
            beta_ref[n] = beta_in[n, 0, 0]

    @pl.when(j > 0)
    def _():
        for h in range(2):
            for q in range(HALF):
                row = jnp.concatenate([block_ref[0, 2 * c + h, :, COLS * q:COLS * q + COLS] for c in range(CHIPS)], axis=1)
                for n in range(ROWS // 8):
                    for t in range(3):
                        tiles[t, pl.ds(8 * PAIR * n + HALF * h + q, 8, stride=PAIR), :] = row[8 * n:8 * n + 8, 128 * t:128 * t + 128]
        for t in range(3):
            out_ref[0, :, 128 * t:128 * t + 128] = tiles[t]


def place_rows(alpha, beta, first, blocks):
    smem = pl.BlockSpec(memory_space=pltpu.SMEM)
    whole = pl.BlockSpec((STEPS, 8, 128), lambda j: (0, 0, 0))
    return pl.pallas_call(
        place_kernel,
        grid=(STEPS + 1,),
        out_shape=(jax.ShapeDtypeStruct((STEPS + 1, ROWS * PAIR, BOND), F32),
                   jax.ShapeDtypeStruct((STEPS,), F32), jax.ShapeDtypeStruct((STEPS,), F32)),
        in_specs=[whole, whole, pl.BlockSpec((ROWS * PAIR, BOND), lambda j: (0, 0)),
                  pl.BlockSpec((1, 16, ROWS, BOND), lambda j: (jnp.maximum(j - 1, 0), 0, 0, 0))],
        out_specs=(pl.BlockSpec((1, ROWS * PAIR, BOND), lambda j: (j, 0, 0)), smem, smem),
        scratch_shapes=[pltpu.VMEM((3, ROWS * PAIR, 128), F32)],
        name='place_rows',
    )(alpha, beta, first, blocks)


def solution(mesh):
    def device_body(psi, left_loc, pair_loc, right_loc, flag_loc):
        blocks, alpha, beta, first = run_steps(psi.reshape(BOND * PAIR, BOND), left_loc, right_loc,
                                               pair_loc.reshape(KLOC * PAIR, PAIR), flag_loc)
        krylov, alpha, beta = place_rows(alpha, beta, first, blocks)
        return krylov.reshape(STEPS + 1, ROWS, PAIR, BOND), alpha, beta

    return jax.shard_map(device_body, mesh=mesh, in_specs=(P(), P(AXIS), P(AXIS), P(AXIS), P(AXIS)),
                         out_specs=(P(None, AXIS), P(), P()), check_vma=False)
```

```python
import jax
import jax.numpy as jnp
from jax import lax
from jax.experimental import pallas as pl
from jax.experimental.pallas import tpu as pltpu
from jax.sharding import PartitionSpec as P

STEPS = 6
AXIS = 'terms'
BOND = 384
PAIR = 16
VEC_SIZE = BOND * PAIR * BOND
CHIPS = 8
COLS = BOND // CHIPS
HALF = PAIR // 2
KLOC = 4
CHUNK = 128
NCHUNK = BOND // CHUNK
QROWS = HALF * COLS
ROWS = BOND // 16
MESH = pl.DeviceIdType.MESH
F32 = jnp.float32
BF16 = jnp.bfloat16
PEERS = (1, 2, 4, 3, 5, 6, 7)
FORWARD_AT = 2


def flip(idx, mask, bits):
    out = 0
    for b in range(bits):
        bit = lax.rem(lax.div(idx, 1 << b), 2)
        if (mask >> b) & 1:
            bit = 1 - bit
        out = out + bit * (1 << b)
    return out


def rotl(pos, chunk):
    if isinstance(pos, int) and isinstance(chunk, int):
        return (pos << chunk) - 7 * ((pos << chunk) // 8)
    scaled = pos * (1 + chunk + lax.div(chunk, 2)) if not isinstance(chunk, int) else pos * (1 << chunk)
    return scaled - 7 * lax.div(scaled, 8)


def kernel(psi_ref, l_ref, r_ref, w_ref, flag_ref,
           kry_ref, alpha_ref, beta_ref, first_ref,
           psi, u, lbuf, rsel, rbuf, wbuf, mbuf, ya, yb, yc, yd, z, sig, sig_in, wv, vcur, vprev, red, norm_v, delta_now, beta_now,
           psi_sem, ll_sem, loc_sem, rs_sem, rr_sem, ws_sem, wr_sem, ls_sem, lr_sem, ns_sem, nr_sem, gs_sem, gr_sem, fs_sem, fr_sem,
           xs_sem, xr_sem, ds_sem, dr_sem, ks_sem, kr_sem, kl_sem):
    me = lax.axis_index(AXIS)
    chip = lax.div(me, 2)
    core = lax.rem(me, 2)
    partner = flip(me, 1, 4)

    def peer(d):
        return flip(chip, d, 3) * 2 + core

    def remote(src, dst, ssem, rsem, dev):
        return pltpu.make_async_remote_copy(src_ref=src, dst_ref=dst, send_sem=ssem, recv_sem=rsem,
                                            device_id=(dev,), device_id_type=MESH)

    l_own = [[pltpu.make_async_copy(l_ref.at[k, :, pl.ds(CHUNK * i, CHUNK)], lbuf.at[i, :, pl.ds(CHUNK * k, CHUNK)], ll_sem.at[i, k])
              for k in range(KLOC)] for i in range(NCHUNK)]
    r_own = pltpu.make_async_copy(r_ref, rsel, loc_sem)
    part_rows = BOND * PAIR // 4
    psi_own = [[pltpu.make_async_copy(psi_ref.at[pl.ds(part_rows * i, part_rows), pl.ds(128 * c, 128)],
                                      psi.at[c, pl.ds(part_rows * i, part_rows)], psi_sem.at[i, c]) for c in range(3)]
               for i in range(4)]
    for i in range(NCHUNK):
        for k in range(KLOC):
            l_own[i][k].start()
    r_own.start()
    for i in range(4):
        for c in range(3):
            psi_own[i][c].start()
    barrier = pltpu.get_barrier_semaphore()
    for d in range(1, 16):
        pl.semaphore_signal(barrier, inc=1, device_id=(flip(me, d, 4),), device_id_type=MESH)
    pl.semaphore_wait(barrier, 15)

    w_copies = {d: remote(w_ref, wbuf.at[d], ws_sem.at[d], wr_sem.at[d], peer(d)) for d in PEERS}
    r_copies = {d: remote(rsel.at[:, pl.ds(pl.multiple_of(COLS * flip(chip, d, 3), 16), COLS)], rbuf.at[d],
                          rs_sem.at[d], rr_sem.at[d], peer(d)) for d in PEERS}

    def l_copies(i, n):
        mask = 1 << ((i + min(n, 2)) % 3)
        src, dst, size = ((0, 512, 512), (0, 1024, 1024), (0, 2048, 1024), (1024, 3072, 1024))[n]
        spans = ((CHUNK * i, 2 * CHUNK),) if i < 2 else ((2 * CHUNK, CHUNK), (0, CHUNK))
        return [remote(lbuf.at[i, pl.ds(row, num), pl.ds(src, size)], lbuf.at[i, pl.ds(row, num), pl.ds(dst, size)],
                       ls_sem.at[i, n, m], lr_sem.at[i, n, m], peer(mask)) for m, (row, num) in enumerate(spans)]

    def l_start(i, n):
        for c in l_copies(i, n):
            c.start()

    def l_wait(i, n):
        for c in l_copies(i, n):
            c.wait_recv()

    for d in PEERS:
        w_copies[d].start()
    for i in range(NCHUNK):
        for k in range(KLOC):
            l_own[i][k].wait()
        l_start(i, 0)

    r_own.wait()
    row_id = lax.broadcasted_iota(jnp.int32, (BOND, BOND), 0)
    col_id = lax.broadcasted_iota(jnp.int32, (BOND, BOND), 1)
    unit = jnp.where(row_id == col_id, 1.0, 0.0).astype(BF16)
    for k in range(KLOC):
        rsel[k] = jnp.where(jnp.full((BOND, BOND), flag_ref[k], jnp.int32) == 1, rsel[k].astype(F32), unit.astype(F32)).astype(BF16)
    for d in PEERS:
        r_copies[d].start()
    rbuf[0] = rsel[:, pl.ds(pl.multiple_of(COLS * chip, 16), COLS), :]

    wbuf[0] = w_ref[...]
    for d in PEERS:
        w_copies[d].wait_recv()
    row_id = lax.broadcasted_iota(jnp.int32, (256, 16), 0)
    col_id = lax.broadcasted_iota(jnp.int32, (256, 16), 1)
    spread = jnp.where(lax.div(row_id, 16) == col_id, 1.0, 0.0).astype(BF16)
    row_id = lax.broadcasted_iota(jnp.int32, (16, 256), 0)
    col_id = lax.broadcasted_iota(jnp.int32, (16, 256), 1)
    spread_t = jnp.where(row_id == lax.div(col_id, 16), 1.0, 0.0).astype(BF16)
    row_id = lax.broadcasted_iota(jnp.int32, (256, 256), 0)
    col_id = lax.broadcasted_iota(jnp.int32, (256, 256), 1)
    same = lax.rem(row_id, 16) == lax.rem(col_id, 16)

    def build(slot, carry):
        for k in range(KLOC):
            tall = jnp.dot(spread, wbuf[slot, pl.ds(16 * k, 16), :], preferred_element_type=F32).astype(BF16)
            full = jnp.dot(tall, spread_t, preferred_element_type=F32)
            mbuf[slot * KLOC + k] = jnp.where(same, full, 0.0).astype(BF16)
        return carry

    lax.fori_loop(0, CHIPS, build, 0)

    def right_part(i, g, y, tiles=range(8)):
        slot_a = rotl(2 * g, i)
        slot_b = rotl(2 * g + 1, i)
        right = jnp.concatenate([rbuf[slot_a].reshape(KLOC * COLS, BOND), rbuf[slot_b].reshape(KLOC * COLS, BOND)], axis=0)
        for n in tiles:
            lanes = pl.ds(256 * n, 256)
            both = jnp.dot(right, u[i, :, lanes], preferred_element_type=F32).astype(BF16)
            y[2 * n] = both[:, 0:128]
            y[2 * n + 1] = both[:, 128:256]

    def pair_part(i, g, y, slot):
        slot_a = rotl(2 * g, i)
        slot_b = rotl(2 * g + 1, i)
        for kk in range(8):
            mat = mbuf[(slot_a if kk < KLOC else slot_b) * KLOC + kk % KLOC]
            cols = [y[:, pl.ds(COLS * kk + 16 * t, 16), :].reshape(PAIR * 16, CHUNK) for t in range(3)]
            pair = jnp.dot(mat, jnp.concatenate(cols, axis=1), preferred_element_type=F32).astype(BF16)
            for t in range(3):
                z[slot, :, pl.ds(16 * t, 16), pl.ds(128 * kk, 128)] = pair[:, 128 * t:128 * t + 128].reshape(PAIR, 16, CHUNK)

    def left_part(i, g, slot):
        left = lbuf[i, :, pl.ds(pl.multiple_of(g * 1024, 1024), 1024)]
        sig[...] += lax.dot_general(left, z[slot].reshape(PAIR * COLS, 2 * KLOC * CHUNK), (((1,), (1,)), ((), ())), preferred_element_type=F32)

    def fold(x):
        out = x[0:8, 0:128]
        for r in range(COLS // 8):
            for c in range(NCHUNK):
                if r or c:
                    out = out + x[8 * r:8 * r + 8, 128 * c:128 * c + 128]
        return out

    def total(x):
        return jnp.sum(x, keepdims=True)

    def vector_part(j):
        lanes = pl.ds(pl.multiple_of(QROWS * core, 128), QROWS)
        other = pl.ds(pl.multiple_of(QROWS * (1 - core), 128), QROWS)
        swaps = [remote(sig.at[pl.ds(96 * n, 96), other], sig_in.at[pl.ds(96 * n, 96)], xs_sem.at[n], xr_sem.at[n], partner)
                 for n in range(4)]
        for c in swaps:
            c.start()
        beta_old = beta_now[0:1, 0:1]
        s_wv = jnp.zeros((8, 128), F32)
        s_cv = jnp.zeros((8, 128), F32)
        for n in range(BOND // COLS):
            if n % 2 == 0:
                swaps[n // 2].wait_recv()
            rows = pl.ds(COLS * n, COLS)
            w = sig[rows, lanes] + sig_in[rows, :]
            v = vcur[rows, :]
            s_wv = s_wv + fold(w * v)
            w = w - beta_old * vprev[rows, :]
            s_cv = s_cv + fold(w * v)
            wv[rows, :] = w
        s_vv = total(norm_v[...])
        guess = jnp.where(s_vv > 0.0, total(s_cv) / jnp.where(s_vv > 0.0, s_vv, 1.0), 0.0)
        s_ww = jnp.zeros((8, 128), F32)
        s_w2v = jnp.zeros((8, 128), F32)
        for n in range(BOND // COLS):
            rows = pl.ds(COLS * n, COLS)
            v = vcur[rows, :]
            w = wv[rows, :] - guess * v
            wv[rows, :] = w
            s_ww = s_ww + fold(w * w)
            s_w2v = s_w2v + fold(w * v)
        row_of = lax.broadcasted_iota(jnp.int32, (8, 128), 0)
        message = jnp.where(row_of == 0, total(s_wv),
                            jnp.where(row_of == 1, guess,
                                      jnp.where(row_of == 2, s_vv, jnp.where(row_of == 3, total(s_ww), total(s_w2v)))))
        phase = lax.rem(j, 2)
        mine = pl.ds(pl.multiple_of(8 * me, 8), 8)
        red[phase, mine, :] = message
        copies = [remote(red.at[phase, mine], red.at[phase, mine], ds_sem.at[phase, d], dr_sem.at[phase, d], flip(me, d, 4))
                  for d in range(1, 16)]
        for c in copies:
            c.start()
        for c in copies:
            c.wait_recv()
        table = red.at[phase]
        a_wv, a_guess, a_vv, a_ww, a_w2v = [table[pl.ds(r, 16, stride=8), :] for r in range(5)]
        alpha = jnp.sum(a_wv, axis=0, keepdims=True) / VEC_SIZE
        shift = alpha - a_guess
        beta = jnp.sqrt(jnp.sum(a_ww - 2.0 * shift * a_w2v + shift * shift * a_vv, axis=0, keepdims=True) / VEC_SIZE)
        beta_now[...] = jnp.broadcast_to(beta, (8, 128))
        delta_now[...] = jnp.broadcast_to(alpha[0:1, 0:1] - guess, (8, 128))
        alpha_ref[j] = jnp.broadcast_to(alpha, (8, 128))
        beta_ref[j] = jnp.broadcast_to(beta, (8, 128))
        norm_v[...] = jnp.zeros_like(norm_v)
        for c in copies:
            c.wait_send()
        for c in swaps:
            c.wait_send()

    def advance(i):
        beta = beta_now[0:1, 0:1]
        delta = delta_now[0:1, 0:1]
        rows = pl.ds(CHUNK * i, CHUNK)
        old = vcur[rows, :]
        new = (wv[rows, :] - delta * old) / beta
        vprev[rows, :] = old
        vcur[rows, :] = new
        square = new * new
        acc = norm_v[...]
        for r in range(CHUNK // 8):
            for c in range(NCHUNK):
                acc = acc + square[8 * r:8 * r + 8, 128 * c:128 * c + 128]
        norm_v[...] = acc
        return new

    def kry_copies(j):
        return [remote(vcur.at[pl.ds(pl.multiple_of(ROWS * flip(me, d, 4), 8), ROWS)], kry_ref.at[j, me],
                       ks_sem.at[d], kr_sem.at[d], flip(me, d, 4)) for d in range(1, 16)]

    def kry_own(j):
        return pltpu.make_async_copy(vcur.at[pl.ds(pl.multiple_of(ROWS * me, 8), ROWS)], kry_ref.at[j, me], kl_sem)

    def kry_start(j):
        kry_own(j).start()
        for c in kry_copies(j):
            c.start()

    def kry_wait(j):
        kry_own(j).wait()
        for c in kry_copies(j):
            c.wait()

    square = jnp.zeros((8, 128), F32)
    for i in range(4):
        for c in range(3):
            psi_own[i][c].wait()

        def add_squares(n, acc, base=i * part_rows):
            for c in range(3):
                x = psi[c, pl.ds(pl.multiple_of(base + COLS * n, COLS), COLS), :]
                x = x * x
                for r in range(COLS // 8):
                    acc = acc + x[8 * r:8 * r + 8, :]
            return acc

        square = lax.fori_loop(0, part_rows // COLS, add_squares, square)
    norm = jnp.sqrt(jnp.sum(square, keepdims=True) / VEC_SIZE)

    def spread_pair(q, carry):
        for i in range(NCHUNK):
            for c in range(NCHUNK):
                x = psi[c, pl.ds(CHUNK * PAIR * i + q, CHUNK, stride=PAIR), :]
                x = (x / norm).T
                u[i, pl.ds(128 * c, 128), pl.ds(pl.multiple_of(CHUNK * q, CHUNK), CHUNK)] = x.astype(BF16)
                wv[pl.ds(128 * c, 128), pl.ds(CHUNK * i, CHUNK)] = x

        @pl.when(lax.div(q, HALF) == core)
        def _():
            sig[pl.ds(pl.multiple_of(COLS * lax.rem(q, HALF), COLS), COLS), 0:BOND] = wv[pl.ds(pl.multiple_of(COLS * chip, COLS), COLS), :]

        return carry

    for i in range(NCHUNK):
        l_wait(i, 0)
        l_start(i, 1)
    lax.fori_loop(0, PAIR, spread_pair, 0)
    start = jnp.zeros((8, 128), F32)
    for i in range(NCHUNK):
        x = sig[:, pl.ds(CHUNK * i, CHUNK)].T
        vcur[pl.ds(CHUNK * i, CHUNK), :] = x
        x = x * x
        for r in range(CHUNK // 8):
            for c in range(NCHUNK):
                start = start + x[8 * r:8 * r + 8, 128 * c:128 * c + 128]
    norm_v[...] = start

    def first_rows(n, carry):
        for c in range(3):
            first_ref[pl.ds(pl.multiple_of(COLS * n, COLS), COLS), pl.ds(128 * c, 128)] = \
                psi[c, pl.ds(pl.multiple_of(ROWS * PAIR * me + COLS * n, COLS), COLS), :] / norm
        return carry

    lax.fori_loop(0, ROWS * PAIR // COLS, first_rows, 0)

    vprev[...] = jnp.zeros_like(vprev)
    beta_now[...] = jnp.zeros_like(beta_now)
    sig[...] = jnp.zeros_like(sig)
    for d in PEERS:
        r_copies[d].wait_recv()

    def front_body(n, carry):
        @pl.when(n == FORWARD_AT)
        def _():
            for i in range(NCHUNK):
                l_wait(i, 1)
                l_start(i, 2)
            for i in range(NCHUNK):
                l_start(i, 3)

        i = lax.div(n, 2)
        g = 2 * lax.rem(n, 2)
        right_part(i, g, ya)
        right_part(i, g + 1, yb)
        pair_part(i, g, ya, 4 * i + g)
        pair_part(i, g + 1, yb, 4 * i + g + 1)
        return carry

    lax.fori_loop(0, 6, front_body, 0)

    def mirror(i, g):
        other = lax.rem(i + 2, 3)
        for k in range(2):
            slot = rotl(2 * g + k, i)
            pos = rotl(slot, lax.rem(3 - other, 3))
            for n in range(KLOC):
                block = lbuf[other, pl.ds(pl.multiple_of(CHUNK * i, CHUNK), CHUNK),
                             pl.ds(pl.multiple_of(CHUNK * (KLOC * pos + n), CHUNK), CHUNK)]
                lbuf[i, pl.ds(pl.multiple_of(CHUNK * other, CHUNK), CHUNK),
                     pl.ds(pl.multiple_of(CHUNK * (KLOC * (2 * g + k) + n), CHUNK), CHUNK)] = block.T

    def back(g):
        def body(i, carry):
            mirror(i, g)
            left_part(i, g, 4 * i + g)
            return carry

        lax.fori_loop(0, NCHUNK, body, 0)

    back(0)
    for i in range(NCHUNK):
        l_wait(i, 2)
    back(2)
    for i in range(NCHUNK):
        l_wait(i, 3)
    back(1)
    back(3)
    for d in PEERS:
        w_copies[d].wait_send()
        r_copies[d].wait_send()
    for i in range(NCHUNK):
        for n in range(4):
            for c in l_copies(i, n):
                c.wait_send()
    vector_part(0)

    units = ((0, 0, 512), (0, 512, 512), (1, 0, 1024), (2, 0, 1024))

    def region(un, mask, lo, width):
        i, first, _ = units[un]
        return u.at[i, pl.ds(pl.multiple_of(COLS * flip(chip, mask, 3), 16), COLS),
                    pl.ds(pl.multiple_of(HALF * CHUNK * core + first + lo, 128), width)]

    def near(un, a):
        own = region(un, 0, 0, units[un][2])
        return remote(own, own, ns_sem.at[un, a], nr_sem.at[un, a], peer(1 << a))

    def far(un):
        own = region(un, 0, 0, units[un][2])
        return remote(own, own, ns_sem.at[un, 3], nr_sem.at[un, 3], peer(7))

    def second(un, a, h):
        half = units[un][2] // 2
        block = region(un, 1 << a, half * h, half)
        return remote(block, block, gs_sem.at[un, 2 * a + h], gr_sem.at[un, 2 * a + h], peer(1 << ((a + 1 + h) % 3)))

    def cross(un, n):
        width = units[un][2]
        if n < 5:
            block = region(un, (0, 1, 2, 4, 7)[n], 0, width)
        else:
            a, h = divmod(n - 5, 2)
            block = region(un, (1 << a) ^ (1 << ((a + 1 + h) % 3)), width // 2 * h, width // 2)
        return remote(block, block, fs_sem.at[un, n], fr_sem.at[un, n], partner)

    def send_out(un):
        for a in range(3):
            near(un, a).start()
        far(un).start()
        cross(un, 0).start()

    def hop(un):
        for a in range(3):
            near(un, a).wait_recv()
            second(un, a, 0).start()
            second(un, a, 1).start()
            cross(un, 1 + a).start()

    def land(un):
        far(un).wait_recv()
        cross(un, 4).start()
        for a in range(3):
            for h in range(2):
                second(un, a, h).wait_recv()
                cross(un, 5 + 2 * a + h).start()

    def ready(un):
        for n in range(11):
            cross(un, n).wait_recv()

    def sent(un):
        for a in range(3):
            near(un, a).wait_send()
        far(un).wait_send()
        for a in range(3):
            for h in range(2):
                second(un, a, h).wait_send()
        for n in range(11):
            cross(un, n).wait_send()

    def publish(i):
        flat = advance(i).astype(BF16).T
        for q in range(HALF):
            u[i, pl.ds(pl.multiple_of(COLS * chip, 16), COLS),
              pl.ds(pl.multiple_of(HALF * CHUNK * core + CHUNK * q, 128), CHUNK)] = flat[COLS * q:COLS * q + COLS, :]

    def step_body(j, carry):
        publish(0)
        send_out(0)
        send_out(1)
        publish(1)
        publish(2)
        sig[...] = jnp.zeros_like(sig)
        hop(0)
        hop(1)
        send_out(2)
        land(0)
        ready(0)
        for g, y in enumerate((ya, yb, yc, yd)):
            right_part(0, g, y, (0, 1, 4, 5))
        land(1)
        ready(1)
        right_part(0, 0, ya, (2, 3, 6, 7))
        right_part(0, 1, yb, (2, 3, 6, 7))
        hop(2)
        send_out(3)
        pair_part(0, 0, ya, 0)
        left_part(0, 0, 0)
        pair_part(0, 1, yb, 1)
        left_part(0, 1, 1)
        right_part(0, 2, yc, (2, 3, 6, 7))
        right_part(0, 3, yd, (2, 3, 6, 7))
        pair_part(0, 2, yc, 0)
        left_part(0, 2, 0)
        land(2)
        pair_part(0, 3, yd, 1)
        left_part(0, 3, 1)
        ready(2)

        def body(n, carry):
            i = lax.div(n, 2)
            g = 2 * lax.rem(n, 2)

            @pl.when(n == 4)
            def _():
                ready(3)

            right_part(i, g, ya)
            right_part(i, g + 1, yb)

            pair_part(i, g, ya, 0)
            left_part(i, g, 0)

            @pl.when(n == 2)
            def _():
                hop(3)

            @pl.when(n == 3)
            def _():
                land(3)
                kry_start(j - 1)

            pair_part(i, g + 1, yb, 1)
            left_part(i, g + 1, 1)
            return carry

        lax.fori_loop(2, 6, body, 0)
        for un in range(4):
            sent(un)
        kry_wait(j - 1)
        vector_part(j)
        return carry

    lax.fori_loop(1, STEPS, step_body, 0)
    for i in range(NCHUNK):
        advance(i)
    kry_start(STEPS - 1)
    kry_wait(STEPS - 1)


def run_steps(psi, left_loc, right_loc, w_in, flag_loc):
    dma = pltpu.SemaphoreType.DMA
    vmem = pl.BlockSpec(memory_space=pltpu.VMEM)
    hbm = pl.BlockSpec(memory_space=pl.ANY)
    return pl.pallas_call(
        kernel,
        out_shape=(jax.ShapeDtypeStruct((STEPS, 16, ROWS, BOND), F32),
                   jax.ShapeDtypeStruct((STEPS, 8, 128), F32),
                   jax.ShapeDtypeStruct((STEPS, 8, 128), F32),
                   jax.ShapeDtypeStruct((ROWS * PAIR, BOND), F32)),
        in_specs=[hbm, hbm, hbm, vmem, pl.BlockSpec(memory_space=pltpu.SMEM)],
        out_specs=(hbm, vmem, vmem, vmem),
        scratch_shapes=[
            pltpu.VMEM((3, BOND * PAIR, 128), F32),
            pltpu.VMEM((NCHUNK, BOND, PAIR * CHUNK), BF16),
            pltpu.VMEM((NCHUNK, BOND, CHIPS * KLOC * CHUNK), BF16),
            pltpu.VMEM((KLOC, BOND, BOND), BF16),
            pltpu.VMEM((CHIPS, KLOC, COLS, BOND), BF16),
            pltpu.VMEM((CHIPS, KLOC * 16, PAIR), BF16),
            pltpu.VMEM((CHIPS * KLOC, 256, 256), BF16),
            pltpu.VMEM((PAIR, 2 * KLOC * COLS, CHUNK), BF16),
            pltpu.VMEM((PAIR, 2 * KLOC * COLS, CHUNK), BF16),
            pltpu.VMEM((PAIR, 2 * KLOC * COLS, CHUNK), BF16),
            pltpu.VMEM((PAIR, 2 * KLOC * COLS, CHUNK), BF16),
            pltpu.VMEM((12, PAIR, COLS, 2 * KLOC * CHUNK), BF16),
            pltpu.VMEM((BOND, PAIR * COLS), F32),
            pltpu.VMEM((BOND, QROWS), F32),
            pltpu.VMEM((BOND, QROWS), F32),
            pltpu.VMEM((BOND, QROWS), F32),
            pltpu.VMEM((BOND, QROWS), F32),
            pltpu.VMEM((2, 16 * 8, 128), F32),
            pltpu.VMEM((8, 128), F32),
            pltpu.VMEM((8, 128), F32),
            pltpu.VMEM((8, 128), F32),
            dma((4, 3)), dma((NCHUNK, KLOC)), dma, dma((8,)), dma((8,)), dma((8,)), dma((8,)),
            dma((NCHUNK, 4, 2)), dma((NCHUNK, 4, 2)),
            dma((4, 4)), dma((4, 4)), dma((4, 6)), dma((4, 6)), dma((4, 11)), dma((4, 11)),
            dma((4,)), dma((4,)), dma((2, 16)), dma((2, 16)), dma((16,)), dma((16,)), dma,
        ],
        compiler_params=pltpu.CompilerParams(collective_id=0, has_side_effects=True, vmem_limit_bytes=60 * 1024 * 1024),
        name='lanczos',
    )(psi, left_loc, right_loc, w_in, flag_loc)


def place_kernel(alpha_in, beta_in, first_ref, block_ref, out_ref, alpha_ref, beta_ref, blocks, rows, tiles, in_sem, out_sem):
    def get(j):
        return pltpu.make_async_copy(block_ref.at[j], blocks.at[j], in_sem.at[j])

    def put(j):
        return pltpu.make_async_copy(rows.at[j], out_ref.at[j], out_sem.at[j])

    first = pltpu.make_async_copy(first_ref, rows.at[0], in_sem.at[STEPS])
    for j in range(STEPS):
        get(j).start()
    first.start()
    for n in range(STEPS):
        alpha_ref[n] = alpha_in[n, 0, 0]
        beta_ref[n] = beta_in[n, 0, 0]

    def body(j, carry):
        get(j).wait()
        for h in range(2):
            for q in range(HALF):
                row = jnp.concatenate([blocks[j, 2 * c + h, :, COLS * q:COLS * q + COLS] for c in range(CHIPS)], axis=1)
                for n in range(ROWS // 8):
                    for t in range(3):
                        tiles[t, pl.ds(8 * PAIR * n + HALF * h + q, 8, stride=PAIR), :] = row[8 * n:8 * n + 8, 128 * t:128 * t + 128]
        for t in range(3):
            rows[j + 1, :, 128 * t:128 * t + 128] = tiles[t]
        put(j + 1).start()
        return carry

    lax.fori_loop(0, STEPS, body, 0)
    first.wait()
    put(0).start()
    for j in range(STEPS + 1):
        put(j).wait()


def place_rows(alpha, beta, first, blocks):
    smem = pl.BlockSpec(memory_space=pltpu.SMEM)
    vmem = pl.BlockSpec(memory_space=pltpu.VMEM)
    hbm = pl.BlockSpec(memory_space=pl.ANY)
    return pl.pallas_call(
        place_kernel,
        out_shape=(jax.ShapeDtypeStruct((STEPS + 1, ROWS * PAIR, BOND), F32),
                   jax.ShapeDtypeStruct((STEPS,), F32), jax.ShapeDtypeStruct((STEPS,), F32)),
        in_specs=[vmem, vmem, hbm, hbm],
        out_specs=(hbm, smem, smem),
        scratch_shapes=[pltpu.VMEM((STEPS, 16, ROWS, BOND), F32), pltpu.VMEM((STEPS + 1, ROWS * PAIR, BOND), F32),
                        pltpu.VMEM((3, ROWS * PAIR, 128), F32),
                        pltpu.SemaphoreType.DMA((STEPS + 1,)), pltpu.SemaphoreType.DMA((STEPS + 1,))],
        compiler_params=pltpu.CompilerParams(vmem_limit_bytes=60 * 1024 * 1024),
        name='place_rows',
    )(alpha, beta, first, blocks)


def solution(mesh):
    def device_body(psi, left_loc, pair_loc, right_loc, flag_loc):
        blocks, alpha, beta, first = run_steps(psi.reshape(BOND * PAIR, BOND), left_loc, right_loc,
                                               pair_loc.reshape(KLOC * PAIR, PAIR), flag_loc)
        krylov, alpha, beta = place_rows(alpha, beta, first, blocks)
        return krylov.reshape(STEPS + 1, ROWS, PAIR, BOND), alpha, beta

    return jax.shard_map(device_body, mesh=mesh, in_specs=(P(), P(AXIS), P(AXIS), P(AXIS), P(AXIS)),
                         out_specs=(P(None, AXIS), P(), P()), check_vma=False)
```
